256 devices in a mesh: row: 16 (over x, z_lo, core), col: 16 (over y, z_hi).
Axes of the slice: x: 4, y: 4, z: 8 (z_hi: 4, z_lo: 2; z = z_hi * 2 + z_lo), core: 2. Of those that a mesh axis runs over, the one named last changes fastest.
Arguments:
- dosage: bfloat16 [1536, 196608], P(None, ('row', 'col')), may hold values from 0 to 2
- zscores: bfloat16 [196608], P(('row', 'col')), may hold values from -18 to 18
- band_reach: int32 [256], replicated, may hold values from 0 to 2, as said below
Outputs:
- ld_tiles: bfloat16 [196608, 3840], P(('row', 'col'))
- smoothed: float32 [196608], P(('row', 'col'))
- quadratic: float32 [], replicated
The draws below stay inside these ranges and needn't reach their ends.
Inputs may be any that keep to these rules, and one draw needn't show every extreme that they name: `band_reach`: the first 3 blocks, the last 3 blocks and some two neighbouring blocks reach 2.
All inputs are finite; a program needn't handle non-finite values.
Results may differ from the reference program's by a relative error of at most 0.0042.
Values may be sent and summed in bfloat16 or wider, within the bound.
A program may use at most 64 MiB of HBM per device.

```python
import math
import jax
import jax.numpy as jnp
from jax import lax

BS = 768
NSAMP = 1536
BAND = 2
NBLOCKS = 256
SNPS = 196608
WIDE = 3840


def draw_dosage(key, part):
    key_freq, key_own = jax.random.split(key, 2)
    frequency = jnp.exp(jax.random.uniform(key_freq, (SNPS,), jnp.float32, math.log(0.05), math.log(0.5)))
    spread = jax.random.uniform(key_own, (NSAMP, SNPS), jnp.float32)
    mixed = spread
    return (4.0 * frequency[None, :] * mixed).astype(jnp.bfloat16)


def draw_zscores(key, part):
    position = jnp.arange(SNPS, dtype=jnp.float32) / (SNPS - 1)
    values = jnp.clip(jax.random.normal(key, (SNPS,), jnp.float32), -6.0, 6.0) * (1.0 + 2.0 * position)
    return values.astype(jnp.bfloat16)


def draw_band_reach(key, part):
    key_base = jax.random.fold_in(key, 11)
    key_place = jax.random.fold_in(key, 12)
    base = jax.random.randint(key_base, (NBLOCKS,), 0, BAND + 1, dtype=jnp.int32)
    place = jax.random.randint(key_place, (), 0, NBLOCKS - 1, dtype=jnp.int32)
    blocks = jnp.arange(NBLOCKS, dtype=jnp.int32)
    chosen = (blocks == place) | (blocks == place + 1)
    chosen = chosen | (blocks <= BAND) | (blocks >= NBLOCKS - 1 - BAND)
    return jnp.where(chosen, jnp.int32(BAND), base)


def setup_inputs(seed: int = 0) -> dict:
    key_list = jax.random.split(jax.random.key(seed), 4)
    dosage = draw_dosage(jax.random.fold_in(key_list[3], 71), 0)
    zscores = draw_zscores(jax.random.fold_in(key_list[3], 71), 0)
    band_reach = draw_band_reach(jax.random.fold_in(key_list[3], 71), 0)
    return {"dosage": dosage, "zscores": zscores, "band_reach": band_reach}


def standardize(dosage):
    values = dosage.astype(jnp.float32)
    column_mean = lax.optimization_barrier(jnp.mean(values, axis=0))
    centered = values - column_mean
    variance = lax.optimization_barrier(jnp.mean(centered * centered, axis=0))
    return (centered * lax.rsqrt(variance + 1e-05)).astype(jnp.bfloat16)

def reference(dosage, zscores, band_reach):
    scaled = standardize(dosage)
    margin = BAND * BS
    padded = jnp.pad(scaled, ((0, 0), (margin, margin)))
    padded_z = jnp.pad(zscores, (margin, margin))
    outside = jnp.full((BAND,), -1, jnp.int32)
    padded_reach = jnp.concatenate([outside, band_reach.astype(jnp.int32), outside])
    offsets = jnp.arange(-BAND, BAND + 1, dtype=jnp.int32)

    def one_block(block):
        start = (block * BS).astype(jnp.int32)
        own_block = lax.dynamic_slice_in_dim(scaled, start, BS, 1)
        near_block = lax.dynamic_slice_in_dim(padded, start, WIDE, 1)
        product = jnp.dot(own_block.T, near_block, preferred_element_type=jnp.float32) / NSAMP
        their_reach = lax.dynamic_slice_in_dim(padded_reach, block.astype(jnp.int32), 2 * BAND + 1, 0)
        own_reach = lax.dynamic_index_in_dim(band_reach, block.astype(jnp.int32), 0, False)
        allowed = (jnp.abs(offsets) <= jnp.minimum(own_reach, their_reach)).astype(jnp.float32)
        masked = product.reshape(BS, 2 * BAND + 1, BS) * allowed[None, :, None]
        tile_rows = masked.reshape(BS, WIDE).astype(jnp.bfloat16)
        near_z = lax.dynamic_slice_in_dim(padded_z, start, WIDE, 0)
        result = jnp.dot(tile_rows, near_z, preferred_element_type=jnp.float32)
        return (tile_rows, result)
    tiles, results = lax.map(one_block, jnp.arange(NBLOCKS, dtype=jnp.int32))
    ld_tiles = tiles.reshape(SNPS, WIDE)
    smoothed = results.reshape(SNPS)
    quadratic = jnp.sum(zscores.astype(jnp.float32) * smoothed) / SNPS
    return (ld_tiles, smoothed, quadratic)
```

```python
import functools

import jax
import jax.numpy as jnp
from jax import lax
from jax.experimental import pallas as pl
from jax.experimental.pallas import tpu as pltpu
from jax.sharding import Mesh
from jax.sharding import PartitionSpec as P

BAND = 2
MESH = pl.DeviceIdType.MESH
CHUNK = 256
STEP = 128
NT = (((1,), (1,)), ((), ()))

GROUPS = (((64, 4),), ((4, 4),), ((16, 2),), ((32, 2), (1, 4)))


def group_members(me, group):
    place, base = 0, me
    for stride, size in group:
        digit = lax.rem(lax.div(me, stride), size)
        base = base - digit * stride
        place = place * size + digit
    total = 1
    for _, size in group:
        total *= size

    def device(index):
        result = base
        for stride, size in reversed(group):
            result = result + lax.rem(index, size) * stride
            index = lax.div(index, size)
        return result

    return place, total, device


def column_stats(source, columns, samples):
    width = columns.size

    def add(step, total):
        rows = pl.ds(pl.multiple_of(step * STEP, STEP), STEP)
        values = source[rows, columns].astype(jnp.float32)
        return total + values.reshape(STEP // 8, 8, width).sum(axis=0)

    zero = jnp.zeros((8, width), jnp.float32)
    total = lax.fori_loop(0, samples // STEP, add, zero)
    mean = jnp.sum(total, axis=0, keepdims=True) / samples

    def add_square(step, total):
        rows = pl.ds(pl.multiple_of(step * STEP, STEP), STEP)
        centered = source[rows, columns].astype(jnp.float32) - mean
        return total + (centered * centered).reshape(STEP // 8, 8, width).sum(axis=0)

    total = lax.fori_loop(0, samples // STEP, add_square, zero)
    variance = jnp.sum(total, axis=0, keepdims=True) / samples
    return mean, lax.rsqrt(variance + 1e-05)


def standardize(source, plain, turned, columns, samples):
    mean, inverse = column_stats(source, columns, samples)

    def write(step, carry):
        rows = pl.ds(pl.multiple_of(step * STEP, STEP), STEP)
        values = (source[rows, columns].astype(jnp.float32) - mean) * inverse
        plain[rows, columns] = values.astype(jnp.bfloat16)
        turned[columns, rows] = values.T.astype(jnp.bfloat16)
        return carry

    lax.fori_loop(0, samples // STEP, write, 0)


def kernel(
    count,
    x_hbm,
    z_ref,
    reach_ref,
    out_hbm,
    smooth_ref,
    quad_ref,
    own,
    rx,
    plain,
    turned,
    middle,
    tx,
    near_z,
    tx_smooth,
    rx_smooth,
    partial,
    slots,
    load_sem,
    send_sem,
    recv_sem,
    z_send,
    z_recv,
    tile_send,
    tile_recv,
    smooth_send,
    smooth_recv,
    sum_send,
    sum_recv,
    store_sem,
):
    me = lax.axis_index("i")
    samples, width = x_hbm.shape
    chunks = width // CHUNK
    left, right = lax.rem(me + count - 1, count), lax.rem(me + 1, count)
    sides = (left, right)
    groups = [group_members(me, group) for group in GROUPS]

    barrier = pltpu.get_barrier_semaphore()
    greeted = 0
    for device in sides:
        pl.semaphore_signal(barrier, inc=1, device_id=(device,), device_id_type=MESH)
        greeted += 1
    for place, total, device in groups:
        for step in range(1, total):
            peer = device(lax.rem(place + step, total))
            pl.semaphore_signal(barrier, inc=1, device_id=(peer,), device_id_type=MESH)
            greeted += 1
    pl.semaphore_wait(barrier, greeted)

    load = pltpu.make_async_copy(x_hbm, own, load_sem)
    load.start()
    pending = []
    chunk_copies = []
    z_copies = []
    for side in range(2):
        copy = pltpu.make_async_remote_copy(
            src_ref=z_ref,
            dst_ref=near_z.at[1 - side],
            send_sem=z_send.at[side],
            recv_sem=z_recv.at[1 - side],
            device_id=(sides[side],),
            device_id_type=MESH,
        )
        copy.start()
        z_copies.append(copy)
    for chunk in range(chunks):
        columns = pl.ds(chunk * CHUNK, CHUNK)
        pair = []
        for side in range(2):
            copy = pltpu.make_async_remote_copy(
                src_ref=x_hbm.at[:, columns],
                dst_ref=rx.at[1 - side, :, columns],
                send_sem=send_sem.at[side, chunk],
                recv_sem=recv_sem.at[1 - side, chunk],
                device_id=(sides[side],),
                device_id_type=MESH,
            )
            copy.start()
            pair.append(copy)
        chunk_copies.append(pair)

    def reach_of(block):
        inside = (block >= 0) & (block < count)
        value = reach_ref[jnp.clip(block, 0, count - 1)]
        return jnp.where(inside, value, -1)

    def factor(first, second, offset):
        allowed = jnp.minimum(reach_of(first), reach_of(second)) >= offset
        return jnp.where(allowed, jnp.float32(1.0), jnp.float32(0.0)) / samples

    near_factor = (factor(me, me - 1, 1), factor(me, me + 1, 1))
    far_factor = factor(me - 1, me + 1, 2)
    own_factor = factor(me, me, 0)

    load.wait()
    for chunk in range(chunks):
        standardize(own, plain.at[2], turned.at[2], pl.ds(chunk * CHUNK, CHUNK), samples)

    def into_middle(slot, columns, place, scale):
        def rows_of(step, carry):
            rows = pl.ds(pl.multiple_of(step * CHUNK, CHUNK), CHUNK)
            product = jnp.dot(
                turned[2, rows, :], plain[slot, :, columns], preferred_element_type=jnp.float32
            )
            middle[rows, place] = (product * scale).astype(jnp.bfloat16)
            return carry

        lax.fori_loop(0, width // CHUNK, rows_of, 0)

    def stored(place, index):
        copy = pltpu.make_async_copy(
            middle.at[:, place],
            out_hbm.at[:, pl.ds(width + place.start, place.size)],
            store_sem.at[index],
        )
        copy.start()
        return copy

    for chunk in range(chunks):
        into_middle(
            2, pl.ds(chunk * CHUNK, CHUNK), pl.ds(width + chunk * CHUNK, CHUNK), own_factor
        )
    stores = [stored(pl.ds(width, width), 1)]

    def tile_copy(side, index, rows, columns):
        place = 4 * width if side == 0 else 0
        return pltpu.make_async_remote_copy(
            src_ref=tx.at[side, rows, columns],
            dst_ref=out_hbm.at[rows, pl.ds(place + columns.start, columns.size)],
            send_sem=tile_send.at[side, index],
            recv_sem=tile_recv.at[1 - side, index],
            device_id=(sides[side],),
            device_id_type=MESH,
        )

    tile_copies = []
    held_back = []
    for chunk in range(chunks):
        columns = pl.ds(chunk * CHUNK, CHUNK)
        for side in range(2):
            chunk_copies[chunk][1 - side].wait_recv()
            standardize(rx.at[side], plain.at[side], turned.at[side], columns, samples)
        pieces = [(columns, pl.ds(0, (chunk + 1) * CHUNK))]
        if chunk:
            pieces.append((pl.ds(0, chunk * CHUNK), columns))
        for index, (rows, across) in enumerate(pieces):
            for side in range(2):
                product = jnp.dot(
                    turned[side, rows, :],
                    plain[1 - side, :, across],
                    preferred_element_type=jnp.float32,
                )
                tx[side, rows, across] = (product * far_factor).astype(jnp.bfloat16)
        for side in range(2):
            into_middle(
                side,
                columns,
                pl.ds(2 * width * side + chunk * CHUNK, CHUNK),
                near_factor[side],
            )
        for index, (rows, across) in enumerate(pieces):
            for side in range(2):
                copy = tile_copy(side, 2 * chunk + index, rows, across)
                tile_copies.append(copy)
                if chunk == chunks - 1 and index == 1:
                    held_back.append(copy)
                else:
                    copy.start()
    stores.append(stored(pl.ds(0, width), 0))
    stores.append(stored(pl.ds(2 * width, width), 2))

    def applied(scores, tile):
        scores = jnp.broadcast_to(scores, (8, width)).astype(jnp.bfloat16)
        return lax.dot_general(scores, tile, NT, preferred_element_type=jnp.float32)[0:1, :]

    own_z = z_ref[...]
    for side in range(2):
        z_copies[side].wait_recv()
    smooth_own = applied(own_z, middle[:, pl.ds(width, width)])
    smooth_left = applied(near_z[0], middle[:, pl.ds(0, width)])
    smooth_right = applied(near_z[1], middle[:, pl.ds(2 * width, width)])
    for side in range(2):
        tx_smooth[side] = applied(near_z[1 - side], tx[side])

    share = own_z * (smooth_own + 2.0 * smooth_right) + 2.0 * near_z[0] * tx_smooth[0]
    total = jnp.sum(share, axis=1, keepdims=True)
    partial[0] = jnp.broadcast_to(total, (8, 128))

    smooth_copies = []
    sum_copies = []
    first_slot = 0
    for index, (place, size, device) in enumerate(groups):
        slots[first_slot + place] = partial[index]
        copies = []
        for step in range(1, size):
            peer = device(lax.rem(place + step, size))
            copy = pltpu.make_async_remote_copy(
                src_ref=partial.at[index],
                dst_ref=slots.at[first_slot + place],
                send_sem=sum_send.at[first_slot + step],
                recv_sem=sum_recv.at[first_slot + step],
                device_id=(peer,),
                device_id_type=MESH,
            )
            copy.start()
            copies.append(copy)
        sum_copies += copies
        if index == len(groups) - 1:
            for side in range(2):
                copy = pltpu.make_async_remote_copy(
                    src_ref=tx_smooth.at[side],
                    dst_ref=rx_smooth.at[1 - side],
                    send_sem=smooth_send.at[side],
                    recv_sem=smooth_recv.at[1 - side],
                    device_id=(sides[side],),
                    device_id_type=MESH,
                )
                copy.start()
                smooth_copies.append(copy)
            for copy in held_back:
                copy.start()
        for copy in copies:
            copy.wait_recv()
        result = slots[first_slot]
        for slot in range(1, size):
            result = result + slots[first_slot + slot]
        if index == len(groups) - 1:
            quad_ref[...] = result / (count * width)
        else:
            partial[index + 1] = result
        first_slot += size

    for copy in smooth_copies:
        copy.wait_recv()
    smooth_ref[...] = (
        smooth_own + smooth_left + smooth_right + rx_smooth[0] + rx_smooth[1]
    )
    for copy in tile_copies:
        copy.wait_recv()
    for store in stores:
        store.wait()
    for pair in chunk_copies:
        for copy in pair:
            copy.wait_send()
    for copy in z_copies + tile_copies + smooth_copies + sum_copies:
        copy.wait_send()


def body(count, dosage, zscores, band_reach):
    samples, width = dosage.shape
    chunks = width // CHUNK
    slots = sum(functools.reduce(lambda a, b: a * b[1], group, 1) for group in GROUPS)
    bf16, f32 = jnp.bfloat16, jnp.float32
    vmem = pl.BlockSpec(memory_space=pltpu.VMEM)
    hbm = pl.BlockSpec(memory_space=pl.ANY)
    ld_tiles, smoothed, quadratic = pl.pallas_call(
        functools.partial(kernel, count),
        out_shape=(
            jax.ShapeDtypeStruct((width, (2 * BAND + 1) * width), bf16),
            jax.ShapeDtypeStruct((1, width), f32),
            jax.ShapeDtypeStruct((8, 128), f32),
        ),
        in_specs=[hbm, vmem, pl.BlockSpec(memory_space=pltpu.SMEM)],
        out_specs=(hbm, vmem, vmem),
        scratch_shapes=[
            pltpu.VMEM((samples, width), bf16),
            pltpu.VMEM((2, samples, width), bf16),
            pltpu.VMEM((3, samples, width), bf16),
            pltpu.VMEM((3, width, samples), bf16),
            pltpu.VMEM((width, 3 * width), bf16),
            pltpu.VMEM((2, width, width), bf16),
            pltpu.VMEM((2, 1, width), f32),
            pltpu.VMEM((2, 1, width), f32),
            pltpu.VMEM((2, 1, width), f32),
            pltpu.VMEM((len(GROUPS), 8, 128), f32),
            pltpu.VMEM((slots, 8, 128), f32),
            pltpu.SemaphoreType.DMA,
            pltpu.SemaphoreType.DMA((2, chunks)),
            pltpu.SemaphoreType.DMA((2, chunks)),
            pltpu.SemaphoreType.DMA((2,)),
            pltpu.SemaphoreType.DMA((2,)),
            pltpu.SemaphoreType.DMA((2, 2 * chunks)),
            pltpu.SemaphoreType.DMA((2, 2 * chunks)),
            pltpu.SemaphoreType.DMA((2,)),
            pltpu.SemaphoreType.DMA((2,)),
            pltpu.SemaphoreType.DMA((slots,)),
            pltpu.SemaphoreType.DMA((slots,)),
            pltpu.SemaphoreType.DMA((3,)),
        ],
        compiler_params=pltpu.CompilerParams(
            collective_id=0, has_side_effects=True, vmem_limit_bytes=60 * 1024 * 1024
        ),
    )(dosage, zscores.astype(f32).reshape(1, width), band_reach)
    return ld_tiles, smoothed.reshape(width), quadratic[0, 0]


def solution(mesh):
    count = mesh.devices.size
    line = Mesh(mesh.devices.reshape(count), ("i",))
    return jax.shard_map(
        functools.partial(body, count),
        mesh=line,
        in_specs=(P(None, "i"), P("i"), P()),
        out_specs=(P("i", None), P("i"), P()),
        check_vma=False,
    )
```

```python
import functools

import jax
import jax.numpy as jnp
from jax import lax
from jax.experimental import pallas as pl
from jax.experimental.pallas import tpu as pltpu
from jax.sharding import Mesh
from jax.sharding import PartitionSpec as P

BAND = 2
MESH = pl.DeviceIdType.MESH
CHUNKS = (256, 256, 128, 128)
ROWS = 256
STEP = 128
WRITES = 6
NT = (((1,), (1,)), ((), ()))

NEAR_STEPS = ((16, 2, "flip"), (32, 2, "flip"), (64, 4, "flip"), (64, 4, "mirror"), (4, 4, "flip"), (4, 4, "mirror"))
STEPS = len(NEAR_STEPS) + 2


def partners_of(me, count):
    partners = []
    for stride, size, kind in NEAR_STEPS:
        digit = lax.rem(lax.div(me, stride), size)
        step = 1 - 2 * lax.rem(digit, 2) if kind == "flip" else size - 1 - 2 * digit
        partners.append(me + step * stride)
    step = 1 - 2 * lax.rem(me, 2)
    partners.append(me + step)
    partners.append(lax.rem(me - step + count, count))
    return partners


def column_stats(source, columns, samples):
    width = columns.size

    def add(step, total):
        rows = pl.ds(pl.multiple_of(step * STEP, STEP), STEP)
        values = source[rows, columns].astype(jnp.float32)
        return total + values.reshape(STEP // 8, 8, width).sum(axis=0)

    zero = jnp.zeros((8, width), jnp.float32)
    total = lax.fori_loop(0, samples // STEP, add, zero)
    mean = jnp.sum(total, axis=0, keepdims=True) / samples

    def add_square(step, total):
        rows = pl.ds(pl.multiple_of(step * STEP, STEP), STEP)
        centered = source[rows, columns].astype(jnp.float32) - mean
        return total + (centered * centered).reshape(STEP // 8, 8, width).sum(axis=0)

    total = lax.fori_loop(0, samples // STEP, add_square, zero)
    variance = jnp.sum(total, axis=0, keepdims=True) / samples
    return mean, lax.rsqrt(variance + 1e-05)


def standardize(source, plain, turned, columns, samples):
    mean, inverse = column_stats(source, columns, samples)

    def write(step, carry):
        rows = pl.ds(pl.multiple_of(step * STEP, STEP), STEP)
        values = (source[rows, columns].astype(jnp.float32) - mean) * inverse
        plain[rows, columns] = values.astype(jnp.bfloat16)
        turned[columns, rows] = values.T.astype(jnp.bfloat16)
        return carry

    lax.fori_loop(0, samples // STEP, write, 0)


def kernel(
    count,
    x_hbm,
    z_hbm,
    reach_hbm,
    out_ref,
    smooth_ref,
    quad_ref,
    own,
    own_scores,
    reach_ref,
    rx,
    plain,
    turned,
    tx,
    left_z,
    right_z,
    own_u,
    near_u,
    tx_smooth,
    rx_smooth,
    partial,
    swapped,
    load_sem,
    send_sem,
    recv_sem,
    z_send,
    z_recv,
    u_send,
    u_recv,
    tile_send,
    tile_recv,
    smooth_send,
    smooth_recv,
    sum_send,
    sum_recv,
):
    me = lax.axis_index("i")
    samples, width = x_hbm.shape
    starts = [sum(CHUNKS[:index]) for index in range(len(CHUNKS))]
    left, right = lax.rem(me + count - 1, count), lax.rem(me + 1, count)
    sides = (left, right)
    partners = partners_of(me, count)

    loads = [
        pltpu.make_async_copy(source, target, load_sem.at[index])
        for index, (source, target) in enumerate(
            ((x_hbm, own), (z_hbm, own_scores), (reach_hbm, reach_ref))
        )
    ]
    for load in loads:
        load.start()
    barrier = pltpu.get_barrier_semaphore()
    peers = sides + tuple(partners[: len(NEAR_STEPS)])
    for device in peers:
        pl.semaphore_signal(barrier, inc=1, device_id=(device,), device_id_type=MESH)
    pl.semaphore_wait(barrier, len(peers))

    def to_side(side, source, target, send, recv):
        return pltpu.make_async_remote_copy(
            src_ref=source,
            dst_ref=target,
            send_sem=send.at[side],
            recv_sem=recv.at[1 - side],
            device_id=(sides[side],),
            device_id_type=MESH,
        )

    def started(copies):
        for copy in copies:
            copy.start()
        return copies

    def chunk_copy(side, chunk):
        columns = pl.ds(starts[chunk], CHUNKS[chunk])
        return pltpu.make_async_remote_copy(
            src_ref=x_hbm.at[:, columns],
            dst_ref=rx.at[1 - side, :, columns],
            send_sem=send_sem.at[side, chunk],
            recv_sem=recv_sem.at[1 - side, chunk],
            device_id=(sides[side],),
            device_id_type=MESH,
        )

    near_z = (left_z, right_z)
    z_copies = started(
        [to_side(side, z_hbm, near_z[1 - side], z_send, z_recv) for side in range(2)]
    )
    chunk_copies = [
        [chunk_copy(side, chunk) for side in range(2)] for chunk in range(len(CHUNKS))
    ]
    started(chunk_copies[0])
    for load in loads:
        load.wait()

    def reach_of(block):
        inside = (block >= 0) & (block < count)
        value = reach_ref[jnp.clip(block, 0, count - 1)]
        return jnp.where(inside, value, -1)

    def factor(first, second, offset):
        allowed = jnp.minimum(reach_of(first), reach_of(second)) >= offset
        return jnp.where(allowed, jnp.float32(1.0), jnp.float32(0.0)) / samples

    near_factor = (factor(me, me - 1, 1), factor(me, me + 1, 1))
    far_factor = factor(me - 1, me + 1, 2)
    own_factor = factor(me, me, 0)

    def as_row(scores):
        return scores[...].astype(jnp.float32).reshape(1, width)

    def as_matrix(scores):
        return jnp.broadcast_to(scores, (8, width)).astype(jnp.bfloat16)

    for start in range(0, width, ROWS):
        standardize(own, plain.at[2], turned.at[2], pl.ds(start, ROWS), samples)
    own_u[...] = jnp.dot(
        as_matrix(as_row(own_scores)), turned[2], preferred_element_type=jnp.float32
    )[0:1, :]

    def into_middle(slot, columns, offset, scale):
        def rows_of(step, carry):
            rows = pl.ds(pl.multiple_of(step * ROWS, ROWS), ROWS)
            product = jnp.dot(
                turned[2, rows, :], plain[slot, :, columns], preferred_element_type=jnp.float32
            )
            place = pl.ds((BAND + offset) * width + columns.start, columns.size)
            out_ref[rows, place] = (product * scale).astype(jnp.bfloat16)
            return carry

        lax.fori_loop(0, width // ROWS, rows_of, 0)

    into_middle(2, pl.ds(0, ROWS), 0, own_factor)
    u_copies = started(
        [to_side(side, own_u, near_u.at[1 - side], u_send, u_recv) for side in range(2)]
    )
    for chunk in range(1, len(CHUNKS) - 1):
        started(chunk_copies[chunk])
    for start in range(ROWS, width, ROWS):
        into_middle(2, pl.ds(start, ROWS), 0, own_factor)

    def sum_copy(step):
        return pltpu.make_async_remote_copy(
            src_ref=partial.at[step],
            dst_ref=swapped.at[step],
            send_sem=sum_send.at[step],
            recv_sem=sum_recv.at[step],
            device_id=(partners[step],),
            device_id_type=MESH,
        )

    sum_copies = [sum_copy(step) for step in range(STEPS)]

    def finish_step(step):
        sum_copies[step].wait_recv()
        partial[step + 1] = partial[step] + swapped[step]

    def tile_copy(side, index, rows, columns):
        place = 2 * BAND * width if side == 0 else 0
        return pltpu.make_async_remote_copy(
            src_ref=tx.at[side, rows, columns],
            dst_ref=out_ref.at[rows, pl.ds(place + columns.start, columns.size)],
            send_sem=tile_send.at[side, index],
            recv_sem=tile_recv.at[1 - side, index],
            device_id=(sides[side],),
            device_id_type=MESH,
        )

    tile_copies = []
    for chunk, (start, size) in enumerate(zip(starts, CHUNKS)):
        columns = pl.ds(start, size)
        for side in range(2):
            chunk_copies[chunk][1 - side].wait_recv()
            standardize(rx.at[side], plain.at[side], turned.at[side], columns, samples)
        pieces = [(columns, pl.ds(0, start + size))]
        if chunk:
            pieces.append((pl.ds(0, start), columns))
        for rows, across in pieces:
            for side in range(2):
                product = jnp.dot(
                    turned[side, rows, :],
                    plain[1 - side, :, across],
                    preferred_element_type=jnp.float32,
                )
                tx[side, rows, across] = (product * far_factor).astype(jnp.bfloat16)
        for side in range(2):
            into_middle(side, columns, 2 * side - 1, near_factor[side])
        if chunk == 0:
            for copy in u_copies:
                copy.wait_recv()
            share = own_u[...] * (own_factor * own_u[...] + 2.0 * near_factor[1] * near_u[1])
            share = share + 2.0 * far_factor * near_u[0] * near_u[1]
            partial[0] = jnp.broadcast_to(jnp.sum(share, axis=1, keepdims=True), (8, 128))
            for step in range(len(NEAR_STEPS)):
                started(sum_copies[step : step + 1])
                finish_step(step)
            started(sum_copies[-2:-1])
            started(chunk_copies[-1])
        tile_copies += started(
            [
                tile_copy(side, 2 * chunk + index, rows, across)
                for index, (rows, across) in enumerate(pieces)
                for side in range(2)
            ]
        )
        if chunk == len(CHUNKS) - 2:
            finish_step(STEPS - 2)
            started(sum_copies[-1:])

    def applied(scores, tile):
        return lax.dot_general(
            as_matrix(scores), tile, NT, preferred_element_type=jnp.float32
        )[0:1, :]

    for copy in z_copies:
        copy.wait_recv()
    near_z = [as_row(scores) for scores in near_z]
    for side in range(2):
        tx_smooth[side] = applied(near_z[1 - side], tx[side])
    row = applied(as_row(own_scores), out_ref[:, pl.ds(BAND * width, width)])
    smooth_copies = started(
        [
            to_side(side, tx_smooth.at[side], rx_smooth.at[1 - side], smooth_send, smooth_recv)
            for side in range(2)
        ]
    )
    for side in range(2):
        place = pl.ds((BAND + 2 * side - 1) * width, width)
        row = row + applied(near_z[side], out_ref[:, place])
    finish_step(STEPS - 1)
    quad_ref[...] = partial[STEPS] / (count * width)
    for copy in smooth_copies:
        copy.wait_recv()
    row = row + rx_smooth[0] + rx_smooth[1]
    smooth_ref[...] = row.reshape(width)
    for copy in tile_copies:
        copy.wait_recv()
    for pair in chunk_copies:
        for copy in pair:
            copy.wait_send()
    for copy in z_copies + u_copies + tile_copies + smooth_copies + sum_copies:
        copy.wait_send()


def finish(tiles_ref, smooth_ref, quad_ref, tiles_hbm, smooth_hbm, quad_out, sems):
    rows = tiles_ref.shape[0] // WRITES
    copies = [pltpu.make_async_copy(smooth_ref, smooth_hbm, sems.at[WRITES])]
    for index in range(WRITES):
        place = pl.ds(index * rows, rows)
        copies.append(
            pltpu.make_async_copy(tiles_ref.at[place], tiles_hbm.at[place], sems.at[index])
        )
    for copy in copies:
        copy.start()
    quad_out[0, 0] = quad_ref[0, 0]
    for copy in copies:
        copy.wait()


def body(count, dosage, zscores, band_reach):
    samples, width = dosage.shape
    chunks = len(CHUNKS)
    bf16, f32 = jnp.bfloat16, jnp.float32
    vmem = pl.BlockSpec(memory_space=pltpu.VMEM)
    hbm = pl.BlockSpec(memory_space=pltpu.HBM)
    smem = pl.BlockSpec(memory_space=pltpu.SMEM)
    placed = pltpu.with_memory_space_constraint
    pair = pltpu.SemaphoreType.DMA((2,))
    results = pl.pallas_call(
        functools.partial(kernel, count),
        out_shape=(
            pltpu.VMEM((width, (2 * BAND + 1) * width), bf16),
            pltpu.VMEM((width,), f32),
            pltpu.VMEM((8, 128), f32),
        ),
        in_specs=[hbm, hbm, hbm],
        out_specs=(vmem, vmem, vmem),
        scratch_shapes=[
            pltpu.VMEM((samples, width), bf16),
            pltpu.VMEM((width,), bf16),
            pltpu.SMEM((count,), jnp.int32),
            pltpu.VMEM((2, samples, width), bf16),
            pltpu.VMEM((3, samples, width), bf16),
            pltpu.VMEM((3, width, samples), bf16),
            pltpu.VMEM((2, width, width), bf16),
            pltpu.VMEM((width,), bf16),
            pltpu.VMEM((width,), bf16),
            pltpu.VMEM((1, samples), f32),
            pltpu.VMEM((2, 1, samples), f32),
            pltpu.VMEM((2, 1, width), f32),
            pltpu.VMEM((2, 1, width), f32),
            pltpu.VMEM((STEPS + 1, 8, 128), f32),
            pltpu.VMEM((STEPS, 8, 128), f32),
            pltpu.SemaphoreType.DMA((3,)),
            pltpu.SemaphoreType.DMA((2, chunks)),
            pltpu.SemaphoreType.DMA((2, chunks)),
            pair,
            pair,
            pair,
            pair,
            pltpu.SemaphoreType.DMA((2, 2 * chunks)),
            pltpu.SemaphoreType.DMA((2, 2 * chunks)),
            pair,
            pair,
            pltpu.SemaphoreType.DMA((STEPS,)),
            pltpu.SemaphoreType.DMA((STEPS,)),
        ],
        compiler_params=pltpu.CompilerParams(
            collective_id=0, has_side_effects=True, vmem_limit_bytes=40 * 1024 * 1024
        ),
    )(*[placed(value, pltpu.HBM) for value in (dosage, zscores, band_reach)])
    ld_tiles, smoothed, quadratic = pl.pallas_call(
        finish,
        out_shape=(
            jax.ShapeDtypeStruct((width, (2 * BAND + 1) * width), bf16),
            jax.ShapeDtypeStruct((width,), f32),
            jax.ShapeDtypeStruct((1, 1), f32),
        ),
        in_specs=[vmem, vmem, vmem],
        out_specs=(hbm, hbm, smem),
        scratch_shapes=[pltpu.SemaphoreType.DMA((WRITES + 1,))],
        compiler_params=pltpu.CompilerParams(vmem_limit_bytes=1024 * 1024),
    )(*[placed(value, pltpu.VMEM) for value in results])
    return ld_tiles, smoothed, quadratic[0, 0]


def solution(mesh):
    count = mesh.devices.size
    line = Mesh(mesh.devices.reshape(count), ("i",))
    return jax.shard_map(
        functools.partial(body, count),
        mesh=line,
        in_specs=(P(None, "i"), P("i"), P()),
        out_specs=(P("i", None), P("i"), P()),
        check_vma=False,
    )
```

```python
import functools

import jax
import jax.numpy as jnp
from jax import lax
from jax.experimental import pallas as pl
from jax.experimental.pallas import tpu as pltpu
from jax.sharding import Mesh
from jax.sharding import PartitionSpec as P

BAND = 2
MESH = pl.DeviceIdType.MESH
CHUNKS = (256, 256, 128, 128)
ROWS = 256
STEP = 128
WRITES = 6
NT = (((1,), (1,)), ((), ()))

NEAR_STEPS = ((16, 2, "flip"), (64, 4, "flip"), (64, 4, "mirror"), (4, 4, "flip"), (4, 4, "mirror"), (32, 2, "flip"))
STEPS = len(NEAR_STEPS) + 2


def partners_of(me, count):
    partners = []
    for stride, size, kind in NEAR_STEPS:
        digit = lax.rem(lax.div(me, stride), size)
        step = 1 - 2 * lax.rem(digit, 2) if kind == "flip" else size - 1 - 2 * digit
        partners.append(me + step * stride)
    step = 1 - 2 * lax.rem(me, 2)
    partners.append(me + step)
    partners.append(lax.rem(me - step + count, count))
    return partners


def column_stats(source, columns, samples):
    width = columns.size

    def add(step, total):
        rows = pl.ds(pl.multiple_of(step * STEP, STEP), STEP)
        values = source[rows, columns].astype(jnp.float32)
        return total + values.reshape(STEP // 8, 8, width).sum(axis=0)

    zero = jnp.zeros((8, width), jnp.float32)
    total = lax.fori_loop(0, samples // STEP, add, zero)
    mean = jnp.sum(total, axis=0, keepdims=True) / samples

    def add_square(step, total):
        rows = pl.ds(pl.multiple_of(step * STEP, STEP), STEP)
        centered = source[rows, columns].astype(jnp.float32) - mean
        return total + (centered * centered).reshape(STEP // 8, 8, width).sum(axis=0)

    total = lax.fori_loop(0, samples // STEP, add_square, zero)
    variance = jnp.sum(total, axis=0, keepdims=True) / samples
    return mean, lax.rsqrt(variance + 1e-05)


def standardize(source, plain, turned, columns, samples):
    mean, inverse = column_stats(source, columns, samples)

    def write(step, carry):
        rows = pl.ds(pl.multiple_of(step * STEP, STEP), STEP)
        values = (source[rows, columns].astype(jnp.float32) - mean) * inverse
        plain[rows, columns] = values.astype(jnp.bfloat16)
        turned[columns, rows] = values.T.astype(jnp.bfloat16)
        return carry

    lax.fori_loop(0, samples // STEP, write, 0)


def kernel(
    count,
    x_hbm,
    z_hbm,
    reach_hbm,
    out_ref,
    smooth_ref,
    quad_ref,
    own,
    own_scores,
    reach_ref,
    rx,
    plain,
    turned,
    tx,
    left_z,
    right_z,
    own_u,
    near_u,
    tx_smooth,
    rx_smooth,
    partial,
    swapped,
    load_sem,
    send_sem,
    recv_sem,
    z_send,
    z_recv,
    u_send,
    u_recv,
    tile_send,
    tile_recv,
    smooth_send,
    smooth_recv,
    sum_send,
    sum_recv,
):
    me = lax.axis_index("i")
    samples, width = x_hbm.shape
    starts = [sum(CHUNKS[:index]) for index in range(len(CHUNKS))]
    left, right = lax.rem(me + count - 1, count), lax.rem(me + 1, count)
    sides = (left, right)
    partners = partners_of(me, count)

    loads = [
        pltpu.make_async_copy(source, target, load_sem.at[index])
        for index, (source, target) in enumerate(
            ((x_hbm, own), (z_hbm, own_scores), (reach_hbm, reach_ref))
        )
    ]
    for load in loads:
        load.start()
    barrier = pltpu.get_barrier_semaphore()
    peers = sides + tuple(partners[: len(NEAR_STEPS)])
    for device in peers:
        pl.semaphore_signal(barrier, inc=1, device_id=(device,), device_id_type=MESH)
    pl.semaphore_wait(barrier, len(peers))

    def to_side(side, source, target, send, recv):
        return pltpu.make_async_remote_copy(
            src_ref=source,
            dst_ref=target,
            send_sem=send.at[side],
            recv_sem=recv.at[1 - side],
            device_id=(sides[side],),
            device_id_type=MESH,
        )

    def started(copies):
        for copy in copies:
            copy.start()
        return copies

    def chunk_copy(side, chunk):
        columns = pl.ds(starts[chunk], CHUNKS[chunk])
        return pltpu.make_async_remote_copy(
            src_ref=x_hbm.at[:, columns],
            dst_ref=rx.at[1 - side, :, columns],
            send_sem=send_sem.at[side, chunk],
            recv_sem=recv_sem.at[1 - side, chunk],
            device_id=(sides[side],),
            device_id_type=MESH,
        )

    near_z = (left_z, right_z)
    z_copies = started(
        [to_side(side, z_hbm, near_z[1 - side], z_send, z_recv) for side in range(2)]
    )
    chunk_copies = [
        [chunk_copy(side, chunk) for side in range(2)] for chunk in range(len(CHUNKS))
    ]
    started(chunk_copies[0])
    for load in loads:
        load.wait()

    def reach_of(block):
        inside = (block >= 0) & (block < count)
        value = reach_ref[jnp.clip(block, 0, count - 1)]
        return jnp.where(inside, value, -1)

    def factor(first, second, offset):
        allowed = jnp.minimum(reach_of(first), reach_of(second)) >= offset
        return jnp.where(allowed, jnp.float32(1.0), jnp.float32(0.0)) / samples

    near_factor = (factor(me, me - 1, 1), factor(me, me + 1, 1))
    far_factor = factor(me - 1, me + 1, 2)
    own_factor = factor(me, me, 0)

    def as_row(scores):
        return scores[...].astype(jnp.float32).reshape(1, width)

    def as_matrix(scores):
        return jnp.broadcast_to(scores, (8, width)).astype(jnp.bfloat16)

    for start in range(0, width, ROWS):
        standardize(own, plain.at[2], turned.at[2], pl.ds(start, ROWS), samples)
    own_u[...] = jnp.dot(
        as_matrix(as_row(own_scores)), turned[2], preferred_element_type=jnp.float32
    )[0:1, :]

    def into_middle(slot, columns, offset, scale):
        def rows_of(step, carry):
            rows = pl.ds(pl.multiple_of(step * ROWS, ROWS), ROWS)
            product = jnp.dot(
                turned[2, rows, :], plain[slot, :, columns], preferred_element_type=jnp.float32
            )
            place = pl.ds((BAND + offset) * width + columns.start, columns.size)
            out_ref[rows, place] = (product * scale).astype(jnp.bfloat16)
            return carry

        lax.fori_loop(0, width // ROWS, rows_of, 0)

    into_middle(2, pl.ds(0, ROWS), 0, own_factor)
    u_copies = started(
        [to_side(side, own_u, near_u.at[1 - side], u_send, u_recv) for side in range(2)]
    )
    for copies in chunk_copies[1:-1]:
        started(copies)
    for start in range(ROWS, width, ROWS):
        into_middle(2, pl.ds(start, ROWS), 0, own_factor)

    def sum_copy(step):
        return pltpu.make_async_remote_copy(
            src_ref=partial.at[step],
            dst_ref=swapped.at[step],
            send_sem=sum_send.at[step],
            recv_sem=sum_recv.at[step],
            device_id=(partners[step],),
            device_id_type=MESH,
        )

    sum_copies = [sum_copy(step) for step in range(STEPS)]

    def finish_step(step):
        sum_copies[step].wait_recv()
        partial[step + 1] = partial[step] + swapped[step]

    def tile_copy(side, index, rows, columns):
        place = 2 * BAND * width if side == 0 else 0
        return pltpu.make_async_remote_copy(
            src_ref=tx.at[side, rows, columns],
            dst_ref=out_ref.at[rows, pl.ds(place + columns.start, columns.size)],
            send_sem=tile_send.at[side, index],
            recv_sem=tile_recv.at[1 - side, index],
            device_id=(sides[side],),
            device_id_type=MESH,
        )

    tile_copies = []
    ready = []
    for chunk, (start, size) in enumerate(zip(starts, CHUNKS)):
        columns = pl.ds(start, size)
        for side in range(2):
            chunk_copies[chunk][1 - side].wait_recv()
            if side == 1 and chunk == len(CHUNKS) - 2:
                finish_step(STEPS - 3)
                started(sum_copies[STEPS - 2 : STEPS - 1])
                tile_copies += started(ready)
                ready = []
            standardize(rx.at[side], plain.at[side], turned.at[side], columns, samples)
        pieces = [(columns, pl.ds(0, start + size))]
        if chunk:
            pieces.append((pl.ds(0, start), columns))
        for rows, across in pieces:
            for side in range(2):
                product = jnp.dot(
                    turned[side, rows, :],
                    plain[1 - side, :, across],
                    preferred_element_type=jnp.float32,
                )
                tx[side, rows, across] = (product * far_factor).astype(jnp.bfloat16)
        ready += [
            tile_copy(side, 2 * chunk + index, rows, across)
            for index, (rows, across) in enumerate(pieces)
            for side in range(2)
        ]
        if chunk < len(CHUNKS) - 1:
            for side in range(2):
                into_middle(side, columns, 2 * side - 1, near_factor[side])
        if chunk == 0:
            for copy in u_copies:
                copy.wait_recv()
            share = own_u[...] * (own_factor * own_u[...] + 2.0 * near_factor[1] * near_u[1])
            share = share + 2.0 * far_factor * near_u[0] * near_u[1]
            partial[0] = jnp.broadcast_to(jnp.sum(share, axis=1, keepdims=True), (8, 128))
            for step in range(STEPS - 3):
                started(sum_copies[step : step + 1])
                finish_step(step)
            started(sum_copies[STEPS - 3 : STEPS - 2])
            started(chunk_copies[-1])
        if chunk == len(CHUNKS) - 2:
            finish_step(STEPS - 2)
            started(sum_copies[STEPS - 1 :])
            tile_copies += started(ready)
            ready = []

    def applied(scores, tile):
        return lax.dot_general(
            as_matrix(scores), tile, NT, preferred_element_type=jnp.float32
        )[0:1, :]

    for copy in z_copies:
        copy.wait_recv()
    near_z = [as_row(scores) for scores in near_z]
    for side in range(2):
        tx_smooth[side] = applied(near_z[1 - side], tx[side])
    smooth_copies = started(
        [
            to_side(side, tx_smooth.at[side], rx_smooth.at[1 - side], smooth_send, smooth_recv)
            for side in range(2)
        ]
    )
    tile_copies += started(ready)
    row = applied(as_row(own_scores), out_ref[:, pl.ds(BAND * width, width)])
    for side in range(2):
        into_middle(side, columns, 2 * side - 1, near_factor[side])
        place = pl.ds((BAND + 2 * side - 1) * width, width)
        row = row + applied(near_z[side], out_ref[:, place])
    finish_step(STEPS - 1)
    quad_ref[...] = partial[STEPS] / (count * width)
    for copy in smooth_copies:
        copy.wait_recv()
    row = row + rx_smooth[0] + rx_smooth[1]
    smooth_ref[...] = row.reshape(width)
    for copy in tile_copies:
        copy.wait_recv()
    for pair in chunk_copies:
        for copy in pair:
            copy.wait_send()
    for copy in z_copies + u_copies + tile_copies + smooth_copies + sum_copies:
        copy.wait_send()


def finish(tiles_ref, smooth_ref, quad_ref, tiles_hbm, smooth_hbm, quad_out, sems):
    rows = tiles_ref.shape[0] // WRITES
    copies = [pltpu.make_async_copy(smooth_ref, smooth_hbm, sems.at[WRITES])]
    for index in range(WRITES):
        place = pl.ds(index * rows, rows)
        copies.append(
            pltpu.make_async_copy(tiles_ref.at[place], tiles_hbm.at[place], sems.at[index])
        )
    for copy in copies:
        copy.start()
    quad_out[0, 0] = quad_ref[0, 0]
    for copy in copies:
        copy.wait()


def body(count, dosage, zscores, band_reach):
    samples, width = dosage.shape
    chunks = len(CHUNKS)
    bf16, f32 = jnp.bfloat16, jnp.float32
    vmem = pl.BlockSpec(memory_space=pltpu.VMEM)
    hbm = pl.BlockSpec(memory_space=pltpu.HBM)
    smem = pl.BlockSpec(memory_space=pltpu.SMEM)
    placed = pltpu.with_memory_space_constraint
    pair = pltpu.SemaphoreType.DMA((2,))
    results = pl.pallas_call(
        functools.partial(kernel, count),
        out_shape=(
            pltpu.VMEM((width, (2 * BAND + 1) * width), bf16),
            pltpu.VMEM((width,), f32),
            pltpu.VMEM((8, 128), f32),
        ),
        in_specs=[hbm, hbm, hbm],
        out_specs=(vmem, vmem, vmem),
        scratch_shapes=[
            pltpu.VMEM((samples, width), bf16),
            pltpu.VMEM((width,), bf16),
            pltpu.SMEM((count,), jnp.int32),
            pltpu.VMEM((2, samples, width), bf16),
            pltpu.VMEM((3, samples, width), bf16),
            pltpu.VMEM((3, width, samples), bf16),
            pltpu.VMEM((2, width, width), bf16),
            pltpu.VMEM((width,), bf16),
            pltpu.VMEM((width,), bf16),
            pltpu.VMEM((1, samples), f32),
            pltpu.VMEM((2, 1, samples), f32),
            pltpu.VMEM((2, 1, width), f32),
            pltpu.VMEM((2, 1, width), f32),
            pltpu.VMEM((STEPS + 1, 8, 128), f32),
            pltpu.VMEM((STEPS, 8, 128), f32),
            pltpu.SemaphoreType.DMA((3,)),
            pltpu.SemaphoreType.DMA((2, chunks)),
            pltpu.SemaphoreType.DMA((2, chunks)),
            pair,
            pair,
            pair,
            pair,
            pltpu.SemaphoreType.DMA((2, 2 * chunks)),
            pltpu.SemaphoreType.DMA((2, 2 * chunks)),
            pair,
            pair,
            pltpu.SemaphoreType.DMA((STEPS,)),
            pltpu.SemaphoreType.DMA((STEPS,)),
        ],
        compiler_params=pltpu.CompilerParams(
            collective_id=0, has_side_effects=True, vmem_limit_bytes=40 * 1024 * 1024
        ),
    )(*[placed(value, pltpu.HBM) for value in (dosage, zscores, band_reach)])
    ld_tiles, smoothed, quadratic = pl.pallas_call(
        finish,
        out_shape=(
            jax.ShapeDtypeStruct((width, (2 * BAND + 1) * width), bf16),
            jax.ShapeDtypeStruct((width,), f32),
            jax.ShapeDtypeStruct((1, 1), f32),
        ),
        in_specs=[vmem, vmem, vmem],
        out_specs=(hbm, hbm, smem),
        scratch_shapes=[pltpu.SemaphoreType.DMA((WRITES + 1,))],
        compiler_params=pltpu.CompilerParams(vmem_limit_bytes=1024 * 1024),
    )(*[placed(value, pltpu.VMEM) for value in results])
    return ld_tiles, smoothed, quadratic[0, 0]


def solution(mesh):
    count = mesh.devices.size
    line = Mesh(mesh.devices.reshape(count), ("i",))
    return jax.shard_map(
        functools.partial(body, count),
        mesh=line,
        in_specs=(P(None, "i"), P("i"), P()),
        out_specs=(P("i", None), P("i"), P()),
        check_vma=False,
    )
```

```python
import functools

import jax
import jax.numpy as jnp
from jax import lax
from jax.experimental import pallas as pl
from jax.experimental.pallas import tpu as pltpu
from jax.sharding import Mesh
from jax.sharding import PartitionSpec as P

BAND = 2
MESH = pl.DeviceIdType.MESH
CHUNKS = (256, 256, 128, 128)
ROWS = 256
STEP = 128
WRITES = 6
NT = (((1,), (1,)), ((), ()))

NEAR_STEPS = ((16, 2, "flip"), (64, 4, "flip"), (64, 4, "mirror"), (4, 4, "flip"), (4, 4, "mirror"), (32, 2, "flip"))
STEPS = len(NEAR_STEPS) + 2


def partners_of(me, count):
    partners = []
    for stride, size, kind in NEAR_STEPS:
        digit = lax.rem(lax.div(me, stride), size)
        step = 1 - 2 * lax.rem(digit, 2) if kind == "flip" else size - 1 - 2 * digit
        partners.append(me + step * stride)
    step = 1 - 2 * lax.rem(me, 2)
    partners.append(me + step)
    partners.append(lax.rem(me - step + count, count))
    return partners


def column_stats(source, columns, samples):
    width = columns.size

    def add(step, total):
        rows = pl.ds(pl.multiple_of(step * STEP, STEP), STEP)
        values = source[rows, columns].astype(jnp.float32)
        return total + values.reshape(STEP // 8, 8, width).sum(axis=0)

    zero = jnp.zeros((8, width), jnp.float32)
    total = lax.fori_loop(0, samples // STEP, add, zero)
    mean = jnp.sum(total, axis=0, keepdims=True) / samples

    def add_square(step, total):
        rows = pl.ds(pl.multiple_of(step * STEP, STEP), STEP)
        centered = source[rows, columns].astype(jnp.float32) - mean
        return total + (centered * centered).reshape(STEP // 8, 8, width).sum(axis=0)

    total = lax.fori_loop(0, samples // STEP, add_square, zero)
    variance = jnp.sum(total, axis=0, keepdims=True) / samples
    return mean, lax.rsqrt(variance + 1e-05)


def standardize(source, plain, turned, columns, samples):
    mean, inverse = column_stats(source, columns, samples)

    def write(step, carry):
        rows = pl.ds(pl.multiple_of(step * STEP, STEP), STEP)
        values = (source[rows, columns].astype(jnp.float32) - mean) * inverse
        plain[rows, columns] = values.astype(jnp.bfloat16)
        turned[columns, rows] = values.T.astype(jnp.bfloat16)
        return carry

    lax.fori_loop(0, samples // STEP, write, 0)


def kernel(
    count,
    x_hbm,
    z_hbm,
    reach_hbm,
    out_ref,
    smooth_ref,
    quad_ref,
    own,
    own_scores,
    reach_ref,
    rx,
    plain,
    turned,
    tx,
    left_z,
    right_z,
    own_u,
    near_u,
    tx_smooth,
    rx_smooth,
    partial,
    swapped,
    load_sem,
    send_sem,
    recv_sem,
    z_send,
    z_recv,
    u_send,
    u_recv,
    tile_send,
    tile_recv,
    smooth_send,
    smooth_recv,
    sum_send,
    sum_recv,
):
    me = lax.axis_index("i")
    samples, width = x_hbm.shape
    starts = [sum(CHUNKS[:index]) for index in range(len(CHUNKS))]
    left, right = lax.rem(me + count - 1, count), lax.rem(me + 1, count)
    sides = (left, right)
    partners = partners_of(me, count)

    loads = [
        pltpu.make_async_copy(source, target, load_sem.at[index])
        for index, (source, target) in enumerate(
            ((x_hbm, own), (z_hbm, own_scores), (reach_hbm, reach_ref))
        )
    ]
    for load in loads:
        load.start()
    barrier = pltpu.get_barrier_semaphore()
    peers = sides + tuple(partners[: len(NEAR_STEPS)])
    for device in peers:
        pl.semaphore_signal(barrier, inc=1, device_id=(device,), device_id_type=MESH)
    pl.semaphore_wait(barrier, len(peers))

    def to_side(side, source, target, send, recv):
        return pltpu.make_async_remote_copy(
            src_ref=source,
            dst_ref=target,
            send_sem=send.at[side],
            recv_sem=recv.at[1 - side],
            device_id=(sides[side],),
            device_id_type=MESH,
        )

    def started(copies):
        for copy in copies:
            copy.start()
        return copies

    def chunk_copy(side, chunk):
        columns = pl.ds(starts[chunk], CHUNKS[chunk])
        return pltpu.make_async_remote_copy(
            src_ref=x_hbm.at[:, columns],
            dst_ref=rx.at[1 - side, :, columns],
            send_sem=send_sem.at[side, chunk],
            recv_sem=recv_sem.at[1 - side, chunk],
            device_id=(sides[side],),
            device_id_type=MESH,
        )

    near_z = (left_z, right_z)
    z_copies = started(
        [to_side(side, z_hbm, near_z[1 - side], z_send, z_recv) for side in range(2)]
    )
    chunk_copies = [
        [chunk_copy(side, chunk) for side in range(2)] for chunk in range(len(CHUNKS))
    ]
    started(chunk_copies[0])
    for load in loads:
        load.wait()

    def reach_of(block):
        inside = (block >= 0) & (block < count)
        value = reach_ref[jnp.clip(block, 0, count - 1)]
        return jnp.where(inside, value, -1)

    def factor(first, second, offset):
        allowed = jnp.minimum(reach_of(first), reach_of(second)) >= offset
        return jnp.where(allowed, jnp.float32(1.0), jnp.float32(0.0)) / samples

    near_factor = (factor(me, me - 1, 1), factor(me, me + 1, 1))
    far_factor = factor(me - 1, me + 1, 2)
    own_factor = factor(me, me, 0)

    def as_row(scores):
        return scores[...].astype(jnp.float32).reshape(1, width)

    def as_matrix(scores):
        return jnp.broadcast_to(scores, (8, width)).astype(jnp.bfloat16)

    for start in range(0, width, ROWS):
        standardize(own, plain.at[2], turned.at[2], pl.ds(start, ROWS), samples)
    own_u[...] = jnp.dot(
        as_matrix(as_row(own_scores)), turned[2], preferred_element_type=jnp.float32
    )[0:1, :]

    def into_middle(slot, columns, offset, scale):
        def rows_of(step, carry):
            rows = pl.ds(pl.multiple_of(step * ROWS, ROWS), ROWS)
            product = jnp.dot(
                turned[2, rows, :], plain[slot, :, columns], preferred_element_type=jnp.float32
            )
            place = pl.ds((BAND + offset) * width + columns.start, columns.size)
            out_ref[rows, place] = (product * scale).astype(jnp.bfloat16)
            return carry

        lax.fori_loop(0, width // ROWS, rows_of, 0)

    into_middle(2, pl.ds(0, ROWS), 0, own_factor)
    u_copies = started(
        [to_side(side, own_u, near_u.at[1 - side], u_send, u_recv) for side in range(2)]
    )
    started(chunk_copies[1])
    for start in range(ROWS, width, ROWS):
        into_middle(2, pl.ds(start, ROWS), 0, own_factor)

    def sum_copy(step):
        return pltpu.make_async_remote_copy(
            src_ref=partial.at[step],
            dst_ref=swapped.at[step],
            send_sem=sum_send.at[step],
            recv_sem=sum_recv.at[step],
            device_id=(partners[step],),
            device_id_type=MESH,
        )

    sum_copies = [sum_copy(step) for step in range(STEPS)]

    def finish_step(step):
        sum_copies[step].wait_recv()
        partial[step + 1] = partial[step] + swapped[step]

    def tile_copy(side, index, rows, columns):
        place = 2 * BAND * width if side == 0 else 0
        return pltpu.make_async_remote_copy(
            src_ref=tx.at[side, rows, columns],
            dst_ref=out_ref.at[rows, pl.ds(place + columns.start, columns.size)],
            send_sem=tile_send.at[side, index],
            recv_sem=tile_recv.at[1 - side, index],
            device_id=(sides[side],),
            device_id_type=MESH,
        )

    tile_copies = []
    ready = []
    for chunk, (start, size) in enumerate(zip(starts, CHUNKS)):
        columns = pl.ds(start, size)
        for side in range(2):
            chunk_copies[chunk][1 - side].wait_recv()
            if chunk < 2 and side == 1:
                started(chunk_copies[chunk + 2])
            standardize(rx.at[side], plain.at[side], turned.at[side], columns, samples)
        pieces = [(columns, pl.ds(0, start + size))]
        if chunk:
            pieces.append((pl.ds(0, start), columns))
        for rows, across in pieces:
            for side in range(2):
                product = jnp.dot(
                    turned[side, rows, :],
                    plain[1 - side, :, across],
                    preferred_element_type=jnp.float32,
                )
                tx[side, rows, across] = (product * far_factor).astype(jnp.bfloat16)
        ready += [
            tile_copy(side, 2 * chunk + index, rows, across)
            for index, (rows, across) in enumerate(pieces)
            for side in range(2)
        ]
        if chunk < len(CHUNKS) - 1:
            for side in range(2):
                into_middle(side, columns, 2 * side - 1, near_factor[side])
        if chunk == 0:
            for copy in u_copies:
                copy.wait_recv()
            share = own_u[...] * (own_factor * own_u[...] + 2.0 * near_factor[1] * near_u[1])
            share = share + 2.0 * far_factor * near_u[0] * near_u[1]
            partial[0] = jnp.broadcast_to(jnp.sum(share, axis=1, keepdims=True), (8, 128))
            for step in range(STEPS - 3):
                started(sum_copies[step : step + 1])
                finish_step(step)
            started(sum_copies[STEPS - 3 : STEPS - 2])
        if chunk == len(CHUNKS) - 2:
            finish_step(STEPS - 3)
            started(sum_copies[STEPS - 2 : STEPS - 1])
        if chunk < len(CHUNKS) - 1:
            tile_copies += started(ready)
            ready = []

    def applied(scores, tile):
        return lax.dot_general(
            as_matrix(scores), tile, NT, preferred_element_type=jnp.float32
        )[0:1, :]

    for copy in z_copies:
        copy.wait_recv()
    near_z = [as_row(scores) for scores in near_z]
    for side in range(2):
        tx_smooth[side] = applied(near_z[1 - side], tx[side])
    smooth_copies = started(
        [
            to_side(side, tx_smooth.at[side], rx_smooth.at[1 - side], smooth_send, smooth_recv)
            for side in range(2)
        ]
    )
    for copy in tile_copies[:6]:
        copy.wait_recv()
    tile_copies += started(ready[:2])
    finish_step(STEPS - 2)
    started(sum_copies[STEPS - 1 :])
    tile_copies += started(ready[2:])
    row = applied(as_row(own_scores), out_ref[:, pl.ds(BAND * width, width)])
    for side in range(2):
        into_middle(side, columns, 2 * side - 1, near_factor[side])
        place = pl.ds((BAND + 2 * side - 1) * width, width)
        row = row + applied(near_z[side], out_ref[:, place])
    finish_step(STEPS - 1)
    quad_ref[...] = partial[STEPS] / (count * width)
    for copy in smooth_copies:
        copy.wait_recv()
    row = row + rx_smooth[0] + rx_smooth[1]
    smooth_ref[...] = row.reshape(width)
    for copy in tile_copies[6:]:
        copy.wait_recv()
    for pair in chunk_copies:
        for copy in pair:
            copy.wait_send()
    for copy in z_copies + u_copies + tile_copies + smooth_copies + sum_copies:
        copy.wait_send()


def finish(tiles_ref, smooth_ref, quad_ref, tiles_hbm, smooth_hbm, quad_hbm, quad, sems):
    rows = tiles_ref.shape[0] // WRITES
    copies = []
    for index in range(WRITES):
        place = pl.ds(index * rows, rows)
        copies.append(
            pltpu.make_async_copy(tiles_ref.at[place], tiles_hbm.at[place], sems.at[index])
        )
    copies.append(pltpu.make_async_copy(smooth_ref, smooth_hbm, sems.at[WRITES]))
    copies.append(pltpu.make_async_copy(quad, quad_hbm, sems.at[WRITES + 1]))
    for copy in copies[:-1]:
        copy.start()
    quad[0, 0] = quad_ref[0, 0]
    copies[-1].start()
    for copy in copies:
        copy.wait()


def body(count, dosage, zscores, band_reach):
    samples, width = dosage.shape
    chunks = len(CHUNKS)
    bf16, f32 = jnp.bfloat16, jnp.float32
    vmem = pl.BlockSpec(memory_space=pltpu.VMEM)
    hbm = pl.BlockSpec(memory_space=pltpu.HBM)
    placed = pltpu.with_memory_space_constraint
    pair = pltpu.SemaphoreType.DMA((2,))
    results = pl.pallas_call(
        functools.partial(kernel, count),
        out_shape=(
            pltpu.VMEM((width, (2 * BAND + 1) * width), bf16),
            pltpu.VMEM((width,), f32),
            pltpu.VMEM((8, 128), f32),
        ),
        in_specs=[hbm, hbm, hbm],
        out_specs=(vmem, vmem, vmem),
        scratch_shapes=[
            pltpu.VMEM((samples, width), bf16),
            pltpu.VMEM((width,), bf16),
            pltpu.SMEM((count,), jnp.int32),
            pltpu.VMEM((2, samples, width), bf16),
            pltpu.VMEM((3, samples, width), bf16),
            pltpu.VMEM((3, width, samples), bf16),
            pltpu.VMEM((2, width, width), bf16),
            pltpu.VMEM((width,), bf16),
            pltpu.VMEM((width,), bf16),
            pltpu.VMEM((1, samples), f32),
            pltpu.VMEM((2, 1, samples), f32),
            pltpu.VMEM((2, 1, width), f32),
            pltpu.VMEM((2, 1, width), f32),
            pltpu.VMEM((STEPS + 1, 8, 128), f32),
            pltpu.VMEM((STEPS, 8, 128), f32),
            pltpu.SemaphoreType.DMA((3,)),
            pltpu.SemaphoreType.DMA((2, chunks)),
            pltpu.SemaphoreType.DMA((2, chunks)),
            pair,
            pair,
            pair,
            pair,
            pltpu.SemaphoreType.DMA((2, 2 * chunks)),
            pltpu.SemaphoreType.DMA((2, 2 * chunks)),
            pair,
            pair,
            pltpu.SemaphoreType.DMA((STEPS,)),
            pltpu.SemaphoreType.DMA((STEPS,)),
        ],
        compiler_params=pltpu.CompilerParams(
            collective_id=0, has_side_effects=True, vmem_limit_bytes=40 * 1024 * 1024
        ),
    )(*[placed(value, pltpu.HBM) for value in (dosage, zscores, band_reach)])
    ld_tiles, smoothed, quadratic = pl.pallas_call(
        finish,
        out_shape=(
            jax.ShapeDtypeStruct((width, (2 * BAND + 1) * width), bf16),
            jax.ShapeDtypeStruct((width,), f32),
            jax.ShapeDtypeStruct((1, 1), f32),
        ),
        in_specs=[vmem, vmem, vmem],
        out_specs=(hbm, hbm, hbm),
        scratch_shapes=[pltpu.SMEM((1, 1), f32), pltpu.SemaphoreType.DMA((WRITES + 2,))],
        compiler_params=pltpu.CompilerParams(vmem_limit_bytes=1024 * 1024),
    )(*[placed(value, pltpu.VMEM) for value in results])
    return ld_tiles, smoothed, quadratic[0, 0]


def solution(mesh):
    count = mesh.devices.size
    line = Mesh(mesh.devices.reshape(count), ("i",))
    return jax.shard_map(
        functools.partial(body, count),
        mesh=line,
        in_specs=(P(None, "i"), P("i"), P()),
        out_specs=(P("i", None), P("i"), P()),
        check_vma=False,
    )
```

```python
import functools

import jax
import jax.numpy as jnp
from jax import lax
from jax.experimental import pallas as pl
from jax.experimental.pallas import tpu as pltpu
from jax.sharding import Mesh
from jax.sharding import PartitionSpec as P

BAND = 2
MESH = pl.DeviceIdType.MESH
CHUNKS = (256, 256, 128, 128)
ROWS = 256
STEP = 128
WRITES = 6
NT = (((1,), (1,)), ((), ()))

NEAR_STEPS = ((16, 2, "flip"), (64, 4, "flip"), (64, 4, "mirror"), (4, 4, "flip"), (4, 4, "mirror"), (32, 2, "flip"))
STEPS = len(NEAR_STEPS) + 2


def partners_of(me, count):
    partners = []
    for stride, size, kind in NEAR_STEPS:
        digit = lax.rem(lax.div(me, stride), size)
        step = 1 - 2 * lax.rem(digit, 2) if kind == "flip" else size - 1 - 2 * digit
        partners.append(me + step * stride)
    step = 1 - 2 * lax.rem(me, 2)
    partners.append(me + step)
    partners.append(lax.rem(me - step + count, count))
    return partners


def column_stats(source, columns, samples):
    width = columns.size

    def add(step, total):
        rows = pl.ds(pl.multiple_of(step * STEP, STEP), STEP)
        values = source[rows, columns].astype(jnp.float32)
        return total + values.reshape(STEP // 8, 8, width).sum(axis=0)

    zero = jnp.zeros((8, width), jnp.float32)
    total = lax.fori_loop(0, samples // STEP, add, zero)
    mean = jnp.sum(total, axis=0, keepdims=True) / samples

    def add_square(step, total):
        rows = pl.ds(pl.multiple_of(step * STEP, STEP), STEP)
        centered = source[rows, columns].astype(jnp.float32) - mean
        return total + (centered * centered).reshape(STEP // 8, 8, width).sum(axis=0)

    total = lax.fori_loop(0, samples // STEP, add_square, zero)
    variance = jnp.sum(total, axis=0, keepdims=True) / samples
    return mean, lax.rsqrt(variance + 1e-05)


def standardize(source, plain, turned, columns, samples):
    mean, inverse = column_stats(source, columns, samples)

    def write(step, carry):
        rows = pl.ds(pl.multiple_of(step * STEP, STEP), STEP)
        values = (source[rows, columns].astype(jnp.float32) - mean) * inverse
        plain[rows, columns] = values.astype(jnp.bfloat16)
        turned[columns, rows] = values.T.astype(jnp.bfloat16)
        return carry

    lax.fori_loop(0, samples // STEP, write, 0)


def kernel(
    count,
    x_hbm,
    z_hbm,
    reach_hbm,
    out_ref,
    smooth_ref,
    quad_ref,
    own,
    own_scores,
    reach_ref,
    rx,
    plain,
    turned,
    tx,
    left_z,
    right_z,
    own_u,
    near_u,
    tx_smooth,
    rx_smooth,
    partial,
    swapped,
    load_sem,
    send_sem,
    recv_sem,
    z_send,
    z_recv,
    u_send,
    u_recv,
    tile_send,
    tile_recv,
    smooth_send,
    smooth_recv,
    sum_send,
    sum_recv,
):
    me = lax.axis_index("i")
    samples, width = x_hbm.shape
    starts = [sum(CHUNKS[:index]) for index in range(len(CHUNKS))]
    left, right = lax.rem(me + count - 1, count), lax.rem(me + 1, count)
    sides = (left, right)
    partners = partners_of(me, count)

    loads = [
        pltpu.make_async_copy(source, target, load_sem.at[index])
        for index, (source, target) in enumerate(
            ((x_hbm, own), (z_hbm, own_scores), (reach_hbm, reach_ref))
        )
    ]
    for load in loads:
        load.start()
    barrier = pltpu.get_barrier_semaphore()
    peers = sides + tuple(partners[: len(NEAR_STEPS)])
    for device in peers:
        pl.semaphore_signal(barrier, inc=1, device_id=(device,), device_id_type=MESH)
    pl.semaphore_wait(barrier, len(peers))

    def to_side(side, source, target, send, recv):
        return pltpu.make_async_remote_copy(
            src_ref=source,
            dst_ref=target,
            send_sem=send.at[side],
            recv_sem=recv.at[1 - side],
            device_id=(sides[side],),
            device_id_type=MESH,
        )

    def started(copies):
        for copy in copies:
            copy.start()
        return copies

    def chunk_copy(side, chunk):
        columns = pl.ds(starts[chunk], CHUNKS[chunk])
        return pltpu.make_async_remote_copy(
            src_ref=x_hbm.at[:, columns],
            dst_ref=rx.at[1 - side, :, columns],
            send_sem=send_sem.at[side, chunk],
            recv_sem=recv_sem.at[1 - side, chunk],
            device_id=(sides[side],),
            device_id_type=MESH,
        )

    near_z = (left_z, right_z)
    z_copies = started(
        [to_side(side, z_hbm, near_z[1 - side], z_send, z_recv) for side in range(2)]
    )
    chunk_copies = [
        [chunk_copy(side, chunk) for side in range(2)] for chunk in range(len(CHUNKS))
    ]
    started(chunk_copies[0])
    for load in loads:
        load.wait()

    def reach_of(block):
        inside = (block >= 0) & (block < count)
        value = reach_ref[jnp.clip(block, 0, count - 1)]
        return jnp.where(inside, value, -1)

    def factor(first, second, offset):
        allowed = jnp.minimum(reach_of(first), reach_of(second)) >= offset
        return jnp.where(allowed, jnp.float32(1.0), jnp.float32(0.0)) / samples

    near_factor = (factor(me, me - 1, 1), factor(me, me + 1, 1))
    far_factor = factor(me - 1, me + 1, 2)
    own_factor = factor(me, me, 0)

    def as_row(scores):
        return scores[...].astype(jnp.float32).reshape(1, width)

    def as_matrix(scores):
        return jnp.broadcast_to(scores, (8, width)).astype(jnp.bfloat16)

    for start in range(0, width, ROWS):
        standardize(own, plain.at[2], turned.at[2], pl.ds(start, ROWS), samples)
    own_u[...] = jnp.dot(
        as_matrix(as_row(own_scores)), turned[2], preferred_element_type=jnp.float32
    )[0:1, :]

    def into_middle(slot, columns, offset, scale):
        def rows_of(step, carry):
            rows = pl.ds(pl.multiple_of(step * ROWS, ROWS), ROWS)
            product = jnp.dot(
                turned[2, rows, :], plain[slot, :, columns], preferred_element_type=jnp.float32
            )
            place = pl.ds((BAND + offset) * width + columns.start, columns.size)
            out_ref[rows, place] = (product * scale).astype(jnp.bfloat16)
            return carry

        lax.fori_loop(0, width // ROWS, rows_of, 0)

    into_middle(2, pl.ds(0, ROWS), 0, own_factor)
    u_copies = started(
        [to_side(side, own_u, near_u.at[1 - side], u_send, u_recv) for side in range(2)]
    )
    started(chunk_copies[1])
    for start in range(ROWS, width, ROWS):
        into_middle(2, pl.ds(start, ROWS), 0, own_factor)

    def sum_copy(step):
        return pltpu.make_async_remote_copy(
            src_ref=partial.at[step],
            dst_ref=swapped.at[step],
            send_sem=sum_send.at[step],
            recv_sem=sum_recv.at[step],
            device_id=(partners[step],),
            device_id_type=MESH,
        )

    sum_copies = [sum_copy(step) for step in range(STEPS)]

    def finish_step(step):
        sum_copies[step].wait_recv()
        partial[step + 1] = partial[step] + swapped[step]

    def tile_copy(side, index, rows, columns):
        place = 2 * BAND * width if side == 0 else 0
        return pltpu.make_async_remote_copy(
            src_ref=tx.at[side, rows, columns],
            dst_ref=out_ref.at[rows, pl.ds(place + columns.start, columns.size)],
            send_sem=tile_send.at[side, index],
            recv_sem=tile_recv.at[1 - side, index],
            device_id=(sides[side],),
            device_id_type=MESH,
        )

    tile_copies = []
    ready = []
    for chunk, (start, size) in enumerate(zip(starts, CHUNKS)):
        columns = pl.ds(start, size)
        for side in range(2):
            chunk_copies[chunk][1 - side].wait_recv()
            if chunk < 2 and side == 1:
                started(chunk_copies[chunk + 2])
            standardize(rx.at[side], plain.at[side], turned.at[side], columns, samples)
        pieces = [(columns, pl.ds(0, start + size))]
        if chunk:
            pieces.append((pl.ds(0, start), columns))
        for rows, across in pieces:
            for side in range(2):
                product = jnp.dot(
                    turned[side, rows, :],
                    plain[1 - side, :, across],
                    preferred_element_type=jnp.float32,
                )
                tx[side, rows, across] = (product * far_factor).astype(jnp.bfloat16)
        ready += [
            tile_copy(side, 2 * chunk + index, rows, across)
            for index, (rows, across) in enumerate(pieces)
            for side in range(2)
        ]
        if chunk < len(CHUNKS) - 1:
            for side in range(2):
                into_middle(side, columns, 2 * side - 1, near_factor[side])
        if chunk == 0:
            for copy in u_copies:
                copy.wait_recv()
            share = own_u[...] * (own_factor * own_u[...] + 2.0 * near_factor[1] * near_u[1])
            share = share + 2.0 * far_factor * near_u[0] * near_u[1]
            partial[0] = jnp.broadcast_to(jnp.sum(share, axis=1, keepdims=True), (8, 128))
            for step in range(STEPS - 3):
                started(sum_copies[step : step + 1])
                finish_step(step)
            started(sum_copies[STEPS - 3 : STEPS - 2])
        if chunk == len(CHUNKS) - 2:
            finish_step(STEPS - 3)
            started(sum_copies[STEPS - 2 : STEPS - 1])
        if chunk < len(CHUNKS) - 1:
            tile_copies += started(ready)
            ready = []

    def applied(scores, tile):
        return lax.dot_general(
            as_matrix(scores), tile, NT, preferred_element_type=jnp.float32
        )[0:1, :]

    for copy in z_copies:
        copy.wait_recv()
    near_z = [as_row(scores) for scores in near_z]
    for side in range(2):
        tx_smooth[side] = applied(near_z[1 - side], tx[side])
    smooth_copies = started(
        [
            to_side(side, tx_smooth.at[side], rx_smooth.at[1 - side], smooth_send, smooth_recv)
            for side in range(2)
        ]
    )
    tile_copies += started(ready[:2])
    finish_step(STEPS - 2)
    started(sum_copies[STEPS - 1 :])
    tile_copies += started(ready[2:])
    row = applied(as_row(own_scores), out_ref[:, pl.ds(BAND * width, width)])
    for side in range(2):
        into_middle(side, columns, 2 * side - 1, near_factor[side])
        place = pl.ds((BAND + 2 * side - 1) * width, width)
        row = row + applied(near_z[side], out_ref[:, place])
    finish_step(STEPS - 1)
    quad_ref[...] = partial[STEPS] / (count * width)
    for copy in smooth_copies:
        copy.wait_recv()
    row = row + rx_smooth[0] + rx_smooth[1]
    smooth_ref[...] = row.reshape(width)
    for copy in tile_copies:
        copy.wait_recv()
    for pair in chunk_copies:
        for copy in pair:
            copy.wait_send()
    for copy in z_copies + u_copies + tile_copies + smooth_copies + sum_copies:
        copy.wait_send()


def finish(tiles_ref, smooth_ref, quad_ref, tiles_hbm, smooth_hbm, quad_hbm, quad, sems):
    rows = tiles_ref.shape[0] // WRITES
    copies = []
    for index in range(WRITES):
        place = pl.ds(index * rows, rows)
        copies.append(
            pltpu.make_async_copy(tiles_ref.at[place], tiles_hbm.at[place], sems.at[index])
        )
    copies.append(pltpu.make_async_copy(smooth_ref, smooth_hbm, sems.at[WRITES]))
    copies.append(pltpu.make_async_copy(quad, quad_hbm, sems.at[WRITES + 1]))
    for copy in copies[:-1]:
        copy.start()
    quad[0, 0] = quad_ref[0, 0]
    copies[-1].start()
    for copy in copies:
        copy.wait()


def body(count, dosage, zscores, band_reach):
    samples, width = dosage.shape
    chunks = len(CHUNKS)
    bf16, f32 = jnp.bfloat16, jnp.float32
    vmem = pl.BlockSpec(memory_space=pltpu.VMEM)
    hbm = pl.BlockSpec(memory_space=pltpu.HBM)
    placed = pltpu.with_memory_space_constraint
    pair = pltpu.SemaphoreType.DMA((2,))
    results = pl.pallas_call(
        functools.partial(kernel, count),
        out_shape=(
            pltpu.VMEM((width, (2 * BAND + 1) * width), bf16),
            pltpu.VMEM((width,), f32),
            pltpu.VMEM((8, 128), f32),
        ),
        in_specs=[hbm, hbm, hbm],
        out_specs=(vmem, vmem, vmem),
        scratch_shapes=[
            pltpu.VMEM((samples, width), bf16),
            pltpu.VMEM((width,), bf16),
            pltpu.SMEM((count,), jnp.int32),
            pltpu.VMEM((2, samples, width), bf16),
            pltpu.VMEM((3, samples, width), bf16),
            pltpu.VMEM((3, width, samples), bf16),
            pltpu.VMEM((2, width, width), bf16),
            pltpu.VMEM((width,), bf16),
            pltpu.VMEM((width,), bf16),
            pltpu.VMEM((1, samples), f32),
            pltpu.VMEM((2, 1, samples), f32),
            pltpu.VMEM((2, 1, width), f32),
            pltpu.VMEM((2, 1, width), f32),
            pltpu.VMEM((STEPS + 1, 8, 128), f32),
            pltpu.VMEM((STEPS, 8, 128), f32),
            pltpu.SemaphoreType.DMA((3,)),
            pltpu.SemaphoreType.DMA((2, chunks)),
            pltpu.SemaphoreType.DMA((2, chunks)),
            pair,
            pair,
            pair,
            pair,
            pltpu.SemaphoreType.DMA((2, 2 * chunks)),
            pltpu.SemaphoreType.DMA((2, 2 * chunks)),
            pair,
            pair,
            pltpu.SemaphoreType.DMA((STEPS,)),
            pltpu.SemaphoreType.DMA((STEPS,)),
        ],
        compiler_params=pltpu.CompilerParams(
            collective_id=0, has_side_effects=True, vmem_limit_bytes=40 * 1024 * 1024
        ),
    )(*[placed(value, pltpu.HBM) for value in (dosage, zscores, band_reach)])
    ld_tiles, smoothed, quadratic = pl.pallas_call(
        finish,
        out_shape=(
            jax.ShapeDtypeStruct((width, (2 * BAND + 1) * width), bf16),
            jax.ShapeDtypeStruct((width,), f32),
            jax.ShapeDtypeStruct((1, 1), f32),
        ),
        in_specs=[vmem, vmem, vmem],
        out_specs=(hbm, hbm, hbm),
        scratch_shapes=[pltpu.SMEM((1, 1), f32), pltpu.SemaphoreType.DMA((WRITES + 2,))],
        compiler_params=pltpu.CompilerParams(vmem_limit_bytes=1024 * 1024),
    )(*[placed(value, pltpu.VMEM) for value in results])
    return ld_tiles, smoothed, quadratic[0, 0]


def solution(mesh):
    count = mesh.devices.size
    line = Mesh(mesh.devices.reshape(count), ("i",))
    return jax.shard_map(
        functools.partial(body, count),
        mesh=line,
        in_specs=(P(None, "i"), P("i"), P()),
        out_specs=(P("i", None), P("i"), P()),
        check_vma=False,
    )
```

```python
import functools

import jax
import jax.numpy as jnp
from jax import lax
from jax.experimental import pallas as pl
from jax.experimental.pallas import tpu as pltpu
from jax.sharding import Mesh
from jax.sharding import PartitionSpec as P

BAND = 2
MESH = pl.DeviceIdType.MESH
CHUNKS = (256, 256, 128, 128)
ROWS = 256
STEP = 128
WRITES = 6
NT = (((1,), (1,)), ((), ()))

NEAR_STEPS = ((16, 2, "flip"), (64, 4, "flip"), (64, 4, "mirror"), (4, 4, "flip"), (4, 4, "mirror"), (32, 2, "flip"))
STEPS = len(NEAR_STEPS) + 2


def partners_of(me, count):
    partners = []
    for stride, size, kind in NEAR_STEPS:
        digit = lax.rem(lax.div(me, stride), size)
        step = 1 - 2 * lax.rem(digit, 2) if kind == "flip" else size - 1 - 2 * digit
        partners.append(me + step * stride)
    step = 1 - 2 * lax.rem(me, 2)
    partners.append(me + step)
    partners.append(lax.rem(me - step + count, count))
    return partners


def column_stats(source, columns, samples):
    width = columns.size

    def add(step, total):
        rows = pl.ds(pl.multiple_of(step * STEP, STEP), STEP)
        values = source[rows, columns].astype(jnp.float32)
        return total + values.reshape(STEP // 8, 8, width).sum(axis=0)

    zero = jnp.zeros((8, width), jnp.float32)
    total = lax.fori_loop(0, samples // STEP, add, zero)
    mean = jnp.sum(total, axis=0, keepdims=True) / samples

    def add_square(step, total):
        rows = pl.ds(pl.multiple_of(step * STEP, STEP), STEP)
        centered = source[rows, columns].astype(jnp.float32) - mean
        return total + (centered * centered).reshape(STEP // 8, 8, width).sum(axis=0)

    total = lax.fori_loop(0, samples // STEP, add_square, zero)
    variance = jnp.sum(total, axis=0, keepdims=True) / samples
    return mean, lax.rsqrt(variance + 1e-05)


def standardize(source, plain, turned, columns, samples):
    mean, inverse = column_stats(source, columns, samples)

    def write(step, carry):
        rows = pl.ds(pl.multiple_of(step * STEP, STEP), STEP)
        values = (source[rows, columns].astype(jnp.float32) - mean) * inverse
        plain[rows, columns] = values.astype(jnp.bfloat16)
        turned[columns, rows] = values.T.astype(jnp.bfloat16)
        return carry

    lax.fori_loop(0, samples // STEP, write, 0)


def kernel(
    count,
    x_hbm,
    z_hbm,
    reach_hbm,
    out_ref,
    smooth_ref,
    quad_ref,
    own,
    own_scores,
    reach_ref,
    rx,
    plain,
    turned,
    tx,
    left_z,
    right_z,
    own_row,
    own_u,
    near_u,
    tx_smooth,
    rx_smooth,
    partial,
    swapped,
    load_sem,
    send_sem,
    recv_sem,
    z_send,
    z_recv,
    u_send,
    u_recv,
    tile_send,
    tile_recv,
    smooth_send,
    smooth_recv,
    sum_send,
    sum_recv,
):
    me = lax.axis_index("i")
    samples, width = x_hbm.shape
    starts = [sum(CHUNKS[:index]) for index in range(len(CHUNKS))]
    left, right = lax.rem(me + count - 1, count), lax.rem(me + 1, count)
    sides = (left, right)
    partners = partners_of(me, count)

    loads = [
        pltpu.make_async_copy(source, target, load_sem.at[index])
        for index, (source, target) in enumerate(
            ((x_hbm, own), (z_hbm, own_scores), (reach_hbm, reach_ref))
        )
    ]
    for load in loads:
        load.start()
    barrier = pltpu.get_barrier_semaphore()
    peers = sides + tuple(partners[: len(NEAR_STEPS)])
    for device in peers:
        pl.semaphore_signal(barrier, inc=1, device_id=(device,), device_id_type=MESH)
    pl.semaphore_wait(barrier, len(peers))

    def to_side(side, source, target, send, recv):
        return pltpu.make_async_remote_copy(
            src_ref=source,
            dst_ref=target,
            send_sem=send.at[side],
            recv_sem=recv.at[1 - side],
            device_id=(sides[side],),
            device_id_type=MESH,
        )

    def started(copies):
        for copy in copies:
            copy.start()
        return copies

    def chunk_copy(side, chunk):
        columns = pl.ds(starts[chunk], CHUNKS[chunk])
        return pltpu.make_async_remote_copy(
            src_ref=x_hbm.at[:, columns],
            dst_ref=rx.at[1 - side, :, columns],
            send_sem=send_sem.at[side, chunk],
            recv_sem=recv_sem.at[1 - side, chunk],
            device_id=(sides[side],),
            device_id_type=MESH,
        )

    near_z = (left_z, right_z)
    z_copies = started(
        [to_side(side, z_hbm, near_z[1 - side], z_send, z_recv) for side in range(2)]
    )
    chunk_copies = [
        [chunk_copy(side, chunk) for side in range(2)] for chunk in range(len(CHUNKS))
    ]
    started(chunk_copies[0])
    for load in loads:
        load.wait()

    def reach_of(block):
        inside = (block >= 0) & (block < count)
        value = reach_ref[jnp.clip(block, 0, count - 1)]
        return jnp.where(inside, value, -1)

    def factor(first, second, offset):
        allowed = jnp.minimum(reach_of(first), reach_of(second)) >= offset
        return jnp.where(allowed, jnp.float32(1.0), jnp.float32(0.0)) / samples

    near_factor = (factor(me, me - 1, 1), factor(me, me + 1, 1))
    far_factor = factor(me - 1, me + 1, 2)
    own_factor = factor(me, me, 0)

    def as_row(scores):
        return scores[...].astype(jnp.float32).reshape(1, width)

    def as_matrix(scores):
        return jnp.broadcast_to(scores, (8, width)).astype(jnp.bfloat16)

    for start in range(0, width, ROWS):
        standardize(own, plain.at[2], turned.at[2], pl.ds(start, ROWS), samples)
    own_u[...] = jnp.dot(
        as_matrix(as_row(own_scores)), turned[2], preferred_element_type=jnp.float32
    )[0:1, :]

    def into_middle(slot, columns, offset, scale):
        def rows_of(step, carry):
            rows = pl.ds(pl.multiple_of(step * ROWS, ROWS), ROWS)
            product = jnp.dot(
                turned[2, rows, :], plain[slot, :, columns], preferred_element_type=jnp.float32
            )
            place = pl.ds((BAND + offset) * width + columns.start, columns.size)
            out_ref[rows, place] = (product * scale).astype(jnp.bfloat16)
            return carry

        lax.fori_loop(0, width // ROWS, rows_of, 0)

    into_middle(2, pl.ds(0, ROWS), 0, own_factor)
    u_copies = started(
        [to_side(side, own_u, near_u.at[1 - side], u_send, u_recv) for side in range(2)]
    )
    started(chunk_copies[1])
    for start in range(ROWS, width, ROWS):
        into_middle(2, pl.ds(start, ROWS), 0, own_factor)

    def applied(scores, tile):
        return lax.dot_general(
            as_matrix(scores), tile, NT, preferred_element_type=jnp.float32
        )[0:1, :]

    own_row[...] = applied(as_row(own_scores), out_ref[:, pl.ds(BAND * width, width)])

    def sum_copy(step):
        return pltpu.make_async_remote_copy(
            src_ref=partial.at[step],
            dst_ref=swapped.at[step],
            send_sem=sum_send.at[step],
            recv_sem=sum_recv.at[step],
            device_id=(partners[step],),
            device_id_type=MESH,
        )

    sum_copies = [sum_copy(step) for step in range(STEPS)]

    def finish_step(step):
        sum_copies[step].wait_recv()
        partial[step + 1] = partial[step] + swapped[step]

    def tile_copy(side, index, rows, columns):
        place = 2 * BAND * width if side == 0 else 0
        return pltpu.make_async_remote_copy(
            src_ref=tx.at[side, rows, columns],
            dst_ref=out_ref.at[rows, pl.ds(place + columns.start, columns.size)],
            send_sem=tile_send.at[side, index],
            recv_sem=tile_recv.at[1 - side, index],
            device_id=(sides[side],),
            device_id_type=MESH,
        )

    tile_copies = []
    ready = []
    for chunk, (start, size) in enumerate(zip(starts, CHUNKS)):
        columns = pl.ds(start, size)
        for side in range(2):
            chunk_copies[chunk][1 - side].wait_recv()
            if chunk < 2 and side == 1:
                started(chunk_copies[chunk + 2])
            standardize(rx.at[side], plain.at[side], turned.at[side], columns, samples)
        pieces = [(columns, pl.ds(0, start + size))]
        if chunk:
            pieces.append((pl.ds(0, start), columns))
        for rows, across in pieces:
            for side in range(2):
                product = jnp.dot(
                    turned[side, rows, :],
                    plain[1 - side, :, across],
                    preferred_element_type=jnp.float32,
                )
                tx[side, rows, across] = (product * far_factor).astype(jnp.bfloat16)
        ready += [
            tile_copy(side, 2 * chunk + index, rows, across)
            for index, (rows, across) in enumerate(pieces)
            for side in range(2)
        ]
        if chunk < len(CHUNKS) - 1:
            for side in range(2):
                into_middle(side, columns, 2 * side - 1, near_factor[side])
        if chunk == 0:
            for copy in u_copies:
                copy.wait_recv()
            share = near_factor[1] * own_u[...] * near_u[1] + far_factor * near_u[0] * near_u[1]
            total = 2.0 * jnp.sum(share, axis=1, keepdims=True)
            total = total + jnp.sum(as_row(own_scores) * own_row[...], axis=1, keepdims=True)
            partial[0] = jnp.broadcast_to(total, (8, 128))
            for step in range(STEPS - 3):
                started(sum_copies[step : step + 1])
                finish_step(step)
            started(sum_copies[STEPS - 3 : STEPS - 2])
        if chunk == len(CHUNKS) - 2:
            finish_step(STEPS - 3)
            started(sum_copies[STEPS - 2 : STEPS - 1])
        if chunk < len(CHUNKS) - 1:
            tile_copies += started(ready)
            ready = []

    for copy in z_copies:
        copy.wait_recv()
    near_z = [as_row(scores) for scores in near_z]
    for side in range(2):
        tx_smooth[side] = applied(near_z[1 - side], tx[side])
    smooth_copies = started(
        [
            to_side(side, tx_smooth.at[side], rx_smooth.at[1 - side], smooth_send, smooth_recv)
            for side in range(2)
        ]
    )
    tile_copies += started(ready[:2])
    finish_step(STEPS - 2)
    started(sum_copies[STEPS - 1 :])
    tile_copies += started(ready[2:])
    row = own_row[...]
    for side in range(2):
        into_middle(side, columns, 2 * side - 1, near_factor[side])
        place = pl.ds((BAND + 2 * side - 1) * width, width)
        row = row + applied(near_z[side], out_ref[:, place])
    finish_step(STEPS - 1)
    quad_ref[...] = partial[STEPS] / (count * width)
    for copy in smooth_copies:
        copy.wait_recv()
    row = row + rx_smooth[0] + rx_smooth[1]
    smooth_ref[...] = row.reshape(width)
    for copy in tile_copies:
        copy.wait_recv()
    for pair in chunk_copies:
        for copy in pair:
            copy.wait_send()
    for copy in z_copies + u_copies + tile_copies + smooth_copies + sum_copies:
        copy.wait_send()


def finish(tiles_ref, smooth_ref, quad_ref, tiles_hbm, smooth_hbm, quad_hbm, quad, sems):
    rows = tiles_ref.shape[0] // WRITES
    copies = []
    for index in range(WRITES):
        place = pl.ds(index * rows, rows)
        copies.append(
            pltpu.make_async_copy(tiles_ref.at[place], tiles_hbm.at[place], sems.at[index])
        )
    copies.append(pltpu.make_async_copy(smooth_ref, smooth_hbm, sems.at[WRITES]))
    copies.append(pltpu.make_async_copy(quad, quad_hbm, sems.at[WRITES + 1]))
    for copy in copies[:-1]:
        copy.start()
    quad[0, 0] = quad_ref[0, 0]
    copies[-1].start()
    for copy in copies:
        copy.wait()


def body(count, dosage, zscores, band_reach):
    samples, width = dosage.shape
    chunks = len(CHUNKS)
    bf16, f32 = jnp.bfloat16, jnp.float32
    vmem = pl.BlockSpec(memory_space=pltpu.VMEM)
    hbm = pl.BlockSpec(memory_space=pltpu.HBM)
    placed = pltpu.with_memory_space_constraint
    pair = pltpu.SemaphoreType.DMA((2,))
    results = pl.pallas_call(
        functools.partial(kernel, count),
        out_shape=(
            pltpu.VMEM((width, (2 * BAND + 1) * width), bf16),
            pltpu.VMEM((width,), f32),
            pltpu.VMEM((8, 128), f32),
        ),
        in_specs=[hbm, hbm, hbm],
        out_specs=(vmem, vmem, vmem),
        scratch_shapes=[
            pltpu.VMEM((samples, width), bf16),
            pltpu.VMEM((width,), bf16),
            pltpu.SMEM((count,), jnp.int32),
            pltpu.VMEM((2, samples, width), bf16),
            pltpu.VMEM((3, samples, width), bf16),
            pltpu.VMEM((3, width, samples), bf16),
            pltpu.VMEM((2, width, width), bf16),
            pltpu.VMEM((width,), bf16),
            pltpu.VMEM((width,), bf16),
            pltpu.VMEM((1, width), f32),
            pltpu.VMEM((1, samples), f32),
            pltpu.VMEM((2, 1, samples), f32),
            pltpu.VMEM((2, 1, width), f32),
            pltpu.VMEM((2, 1, width), f32),
            pltpu.VMEM((STEPS + 1, 8, 128), f32),
            pltpu.VMEM((STEPS, 8, 128), f32),
            pltpu.SemaphoreType.DMA((3,)),
            pltpu.SemaphoreType.DMA((2, chunks)),
            pltpu.SemaphoreType.DMA((2, chunks)),
            pair,
            pair,
            pair,
            pair,
            pltpu.SemaphoreType.DMA((2, 2 * chunks)),
            pltpu.SemaphoreType.DMA((2, 2 * chunks)),
            pair,
            pair,
            pltpu.SemaphoreType.DMA((STEPS,)),
            pltpu.SemaphoreType.DMA((STEPS,)),
        ],
        compiler_params=pltpu.CompilerParams(
            collective_id=0, has_side_effects=True, vmem_limit_bytes=40 * 1024 * 1024
        ),
    )(*[placed(value, pltpu.HBM) for value in (dosage, zscores, band_reach)])
    ld_tiles, smoothed, quadratic = pl.pallas_call(
        finish,
        out_shape=(
            jax.ShapeDtypeStruct((width, (2 * BAND + 1) * width), bf16),
            jax.ShapeDtypeStruct((width,), f32),
            jax.ShapeDtypeStruct((1, 1), f32),
        ),
        in_specs=[vmem, vmem, vmem],
        out_specs=(hbm, hbm, hbm),
        scratch_shapes=[pltpu.SMEM((1, 1), f32), pltpu.SemaphoreType.DMA((WRITES + 2,))],
        compiler_params=pltpu.CompilerParams(vmem_limit_bytes=1024 * 1024),
    )(*[placed(value, pltpu.VMEM) for value in results])
    return ld_tiles, smoothed, quadratic[0, 0]


def solution(mesh):
    count = mesh.devices.size
    line = Mesh(mesh.devices.reshape(count), ("i",))
    return jax.shard_map(
        functools.partial(body, count),
        mesh=line,
        in_specs=(P(None, "i"), P("i"), P()),
        out_specs=(P("i", None), P("i"), P()),
        check_vma=False,
    )
```

```python
import functools

import jax
import jax.numpy as jnp
from jax import lax
from jax.experimental import pallas as pl
from jax.experimental.pallas import tpu as pltpu
from jax.sharding import Mesh
from jax.sharding import PartitionSpec as P

BAND = 2
MESH = pl.DeviceIdType.MESH
CHUNKS = (256, 256, 128, 128)
ROWS = 256
STEP = 128
WRITES = 6
NT = (((1,), (1,)), ((), ()))

NEAR_STEPS = ((16, 2, "flip"), (64, 4, "flip"), (64, 4, "mirror"), (4, 4, "flip"), (4, 4, "mirror"), (32, 2, "flip"))
STEPS = len(NEAR_STEPS) + 2


def partners_of(me, count):
    partners = []
    for stride, size, kind in NEAR_STEPS:
        digit = lax.rem(lax.div(me, stride), size)
        step = 1 - 2 * lax.rem(digit, 2) if kind == "flip" else size - 1 - 2 * digit
        partners.append(me + step * stride)
    step = 1 - 2 * lax.rem(me, 2)
    partners.append(me + step)
    partners.append(lax.rem(me - step + count, count))
    return partners


def column_stats(source, columns, samples):
    width = columns.size

    def add(step, total):
        rows = pl.ds(pl.multiple_of(step * STEP, STEP), STEP)
        values = source[rows, columns].astype(jnp.float32)
        return total + values.reshape(STEP // 8, 8, width).sum(axis=0)

    zero = jnp.zeros((8, width), jnp.float32)
    total = lax.fori_loop(0, samples // STEP, add, zero)
    mean = jnp.sum(total, axis=0, keepdims=True) / samples

    def add_square(step, total):
        rows = pl.ds(pl.multiple_of(step * STEP, STEP), STEP)
        centered = source[rows, columns].astype(jnp.float32) - mean
        return total + (centered * centered).reshape(STEP // 8, 8, width).sum(axis=0)

    total = lax.fori_loop(0, samples // STEP, add_square, zero)
    variance = jnp.sum(total, axis=0, keepdims=True) / samples
    return mean, lax.rsqrt(variance + 1e-05)


def standardize(source, plain, turned, columns, samples):
    mean, inverse = column_stats(source, columns, samples)

    def write(step, carry):
        rows = pl.ds(pl.multiple_of(step * STEP, STEP), STEP)
        values = (source[rows, columns].astype(jnp.float32) - mean) * inverse
        plain[rows, columns] = values.astype(jnp.bfloat16)
        turned[columns, rows] = values.T.astype(jnp.bfloat16)
        return carry

    lax.fori_loop(0, samples // STEP, write, 0)


def kernel(
    count,
    x_hbm,
    z_hbm,
    reach_hbm,
    out_ref,
    smooth_ref,
    quad_ref,
    own,
    own_scores,
    reach_ref,
    rx,
    plain,
    turned,
    tx,
    left_z,
    right_z,
    own_row,
    own_u,
    near_u,
    tx_smooth,
    rx_smooth,
    partial,
    swapped,
    load_sem,
    send_sem,
    recv_sem,
    z_send,
    z_recv,
    u_send,
    u_recv,
    tile_send,
    tile_recv,
    smooth_send,
    smooth_recv,
    sum_send,
    sum_recv,
):
    me = lax.axis_index("i")
    samples, width = x_hbm.shape
    starts = [sum(CHUNKS[:index]) for index in range(len(CHUNKS))]
    left, right = lax.rem(me + count - 1, count), lax.rem(me + 1, count)
    sides = (left, right)
    partners = partners_of(me, count)

    loads = [
        pltpu.make_async_copy(source, target, load_sem.at[index])
        for index, (source, target) in enumerate(
            ((x_hbm, own), (z_hbm, own_scores), (reach_hbm, reach_ref))
        )
    ]
    for load in loads:
        load.start()
    barrier = pltpu.get_barrier_semaphore()
    peers = sides + tuple(partners[: len(NEAR_STEPS)])
    for device in peers:
        pl.semaphore_signal(barrier, inc=1, device_id=(device,), device_id_type=MESH)
    pl.semaphore_wait(barrier, len(peers))

    def to_side(side, source, target, send, recv):
        return pltpu.make_async_remote_copy(
            src_ref=source,
            dst_ref=target,
            send_sem=send.at[side],
            recv_sem=recv.at[1 - side],
            device_id=(sides[side],),
            device_id_type=MESH,
        )

    def started(copies):
        for copy in copies:
            copy.start()
        return copies

    def chunk_copy(side, chunk):
        columns = pl.ds(starts[chunk], CHUNKS[chunk])
        return pltpu.make_async_remote_copy(
            src_ref=x_hbm.at[:, columns],
            dst_ref=rx.at[1 - side, :, columns],
            send_sem=send_sem.at[side, chunk],
            recv_sem=recv_sem.at[1 - side, chunk],
            device_id=(sides[side],),
            device_id_type=MESH,
        )

    near_z = (left_z, right_z)
    z_copies = started(
        [to_side(side, z_hbm, near_z[1 - side], z_send, z_recv) for side in range(2)]
    )
    chunk_copies = [
        [chunk_copy(side, chunk) for side in range(2)] for chunk in range(len(CHUNKS))
    ]
    started(chunk_copies[0])
    for load in loads:
        load.wait()

    def reach_of(block):
        inside = (block >= 0) & (block < count)
        value = reach_ref[jnp.clip(block, 0, count - 1)]
        return jnp.where(inside, value, -1)

    def factor(first, second, offset):
        allowed = jnp.minimum(reach_of(first), reach_of(second)) >= offset
        return jnp.where(allowed, jnp.float32(1.0), jnp.float32(0.0)) / samples

    near_factor = (factor(me, me - 1, 1), factor(me, me + 1, 1))
    far_factor = factor(me - 1, me + 1, 2)
    own_factor = factor(me, me, 0)

    def as_row(scores):
        return scores[...].astype(jnp.float32).reshape(1, width)

    def as_matrix(scores):
        return jnp.broadcast_to(scores, (8, width)).astype(jnp.bfloat16)

    for start in range(0, width, ROWS):
        standardize(own, plain.at[2], turned.at[2], pl.ds(start, ROWS), samples)
    own_u[...] = jnp.dot(
        as_matrix(as_row(own_scores)), turned[2], preferred_element_type=jnp.float32
    )[0:1, :]

    def into_middle(slot, columns, offset, scale):
        def rows_of(step, carry):
            rows = pl.ds(pl.multiple_of(step * ROWS, ROWS), ROWS)
            product = jnp.dot(
                turned[2, rows, :], plain[slot, :, columns], preferred_element_type=jnp.float32
            )
            place = pl.ds((BAND + offset) * width + columns.start, columns.size)
            out_ref[rows, place] = (product * scale).astype(jnp.bfloat16)
            return carry

        lax.fori_loop(0, width // ROWS, rows_of, 0)

    into_middle(2, pl.ds(0, ROWS), 0, own_factor)
    u_copies = started(
        [to_side(side, own_u, near_u.at[1 - side], u_send, u_recv) for side in range(2)]
    )
    started(chunk_copies[1])
    for start in range(ROWS, width, ROWS):
        into_middle(2, pl.ds(start, ROWS), 0, own_factor)

    def applied(scores, tile):
        return lax.dot_general(
            as_matrix(scores), tile, NT, preferred_element_type=jnp.float32
        )[0:1, :]

    own_row[...] = applied(as_row(own_scores), out_ref[:, pl.ds(BAND * width, width)])

    def sum_copy(step):
        return pltpu.make_async_remote_copy(
            src_ref=partial.at[step],
            dst_ref=swapped.at[step],
            send_sem=sum_send.at[step],
            recv_sem=sum_recv.at[step],
            device_id=(partners[step],),
            device_id_type=MESH,
        )

    sum_copies = [sum_copy(step) for step in range(STEPS)]

    def finish_step(step):
        sum_copies[step].wait_recv()
        partial[step + 1] = partial[step] + swapped[step]

    def tile_copy(side, index, rows, columns):
        place = 2 * BAND * width if side == 0 else 0
        return pltpu.make_async_remote_copy(
            src_ref=tx.at[side, rows, columns],
            dst_ref=out_ref.at[rows, pl.ds(place + columns.start, columns.size)],
            send_sem=tile_send.at[side, index],
            recv_sem=tile_recv.at[1 - side, index],
            device_id=(sides[side],),
            device_id_type=MESH,
        )

    tile_copies = []
    ready = []
    for chunk, (start, size) in enumerate(zip(starts, CHUNKS)):
        columns = pl.ds(start, size)
        for side in range(2):
            chunk_copies[chunk][1 - side].wait_recv()
            if chunk < 2 and side == 1:
                started(chunk_copies[chunk + 2])
            standardize(rx.at[side], plain.at[side], turned.at[side], columns, samples)
        pieces = [(columns, pl.ds(0, start + size))]
        if chunk:
            pieces.append((pl.ds(0, start), columns))
        for rows, across in pieces:
            for side in range(2):
                product = jnp.dot(
                    turned[side, rows, :],
                    plain[1 - side, :, across],
                    preferred_element_type=jnp.float32,
                )
                tx[side, rows, across] = (product * far_factor).astype(jnp.bfloat16)
        ready += [
            tile_copy(side, 2 * chunk + index, rows, across)
            for index, (rows, across) in enumerate(pieces)
            for side in range(2)
        ]
        if chunk < len(CHUNKS) - 1:
            for side in range(2):
                into_middle(side, columns, 2 * side - 1, near_factor[side])
        if chunk == 0:
            for copy in u_copies:
                copy.wait_recv()
            share = near_factor[1] * own_u[...] * near_u[1] + far_factor * near_u[0] * near_u[1]
            total = 2.0 * jnp.sum(share, axis=1, keepdims=True)
            total = total + jnp.sum(as_row(own_scores) * own_row[...], axis=1, keepdims=True)
            partial[0] = jnp.broadcast_to(total, (8, 128))
            started(sum_copies[:1])
        if chunk == 1:
            finish_step(0)
            for step in range(1, STEPS - 3):
                started(sum_copies[step : step + 1])
                finish_step(step)
            started(sum_copies[STEPS - 3 : STEPS - 2])
        if chunk == len(CHUNKS) - 2:
            finish_step(STEPS - 3)
            started(sum_copies[STEPS - 2 : STEPS - 1])
        if chunk < len(CHUNKS) - 1:
            tile_copies += started(ready)
            ready = []

    for copy in z_copies:
        copy.wait_recv()
    near_z = [as_row(scores) for scores in near_z]
    for side in range(2):
        tx_smooth[side] = applied(near_z[1 - side], tx[side])
    smooth_copies = started(
        [
            to_side(side, tx_smooth.at[side], rx_smooth.at[1 - side], smooth_send, smooth_recv)
            for side in range(2)
        ]
    )
    tile_copies += started(ready[:2])
    finish_step(STEPS - 2)
    started(sum_copies[STEPS - 1 :])
    tile_copies += started(ready[2:])
    row = own_row[...]
    for side in range(2):
        into_middle(side, columns, 2 * side - 1, near_factor[side])
        place = pl.ds((BAND + 2 * side - 1) * width, width)
        row = row + applied(near_z[side], out_ref[:, place])
    finish_step(STEPS - 1)
    quad_ref[...] = partial[STEPS] / (count * width)
    for copy in smooth_copies:
        copy.wait_recv()
    row = row + rx_smooth[0] + rx_smooth[1]
    smooth_ref[...] = row.reshape(width)
    for copy in tile_copies:
        copy.wait_recv()
    for pair in chunk_copies:
        for copy in pair:
            copy.wait_send()
    for copy in z_copies + u_copies + tile_copies + smooth_copies + sum_copies:
        copy.wait_send()


def finish(tiles_ref, smooth_ref, quad_ref, tiles_hbm, smooth_hbm, quad_hbm, quad, sems):
    rows = tiles_ref.shape[0] // WRITES
    copies = []
    for index in range(WRITES):
        place = pl.ds(index * rows, rows)
        copies.append(
            pltpu.make_async_copy(tiles_ref.at[place], tiles_hbm.at[place], sems.at[index])
        )
    copies.append(pltpu.make_async_copy(smooth_ref, smooth_hbm, sems.at[WRITES]))
    copies.append(pltpu.make_async_copy(quad, quad_hbm, sems.at[WRITES + 1]))
    for copy in copies[:-1]:
        copy.start()
    quad[0, 0] = quad_ref[0, 0]
    copies[-1].start()
    for copy in copies:
        copy.wait()


def body(count, dosage, zscores, band_reach):
    samples, width = dosage.shape
    chunks = len(CHUNKS)
    bf16, f32 = jnp.bfloat16, jnp.float32
    vmem = pl.BlockSpec(memory_space=pltpu.VMEM)
    hbm = pl.BlockSpec(memory_space=pltpu.HBM)
    placed = pltpu.with_memory_space_constraint
    pair = pltpu.SemaphoreType.DMA((2,))
    results = pl.pallas_call(
        functools.partial(kernel, count),
        out_shape=(
            pltpu.VMEM((width, (2 * BAND + 1) * width), bf16),
            pltpu.VMEM((width,), f32),
            pltpu.VMEM((8, 128), f32),
        ),
        in_specs=[hbm, hbm, hbm],
        out_specs=(vmem, vmem, vmem),
        scratch_shapes=[
            pltpu.VMEM((samples, width), bf16),
            pltpu.VMEM((width,), bf16),
            pltpu.SMEM((count,), jnp.int32),
            pltpu.VMEM((2, samples, width), bf16),
            pltpu.VMEM((3, samples, width), bf16),
            pltpu.VMEM((3, width, samples), bf16),
            pltpu.VMEM((2, width, width), bf16),
            pltpu.VMEM((width,), bf16),
            pltpu.VMEM((width,), bf16),
            pltpu.VMEM((1, width), f32),
            pltpu.VMEM((1, samples), f32),
            pltpu.VMEM((2, 1, samples), f32),
            pltpu.VMEM((2, 1, width), f32),
            pltpu.VMEM((2, 1, width), f32),
            pltpu.VMEM((STEPS + 1, 8, 128), f32),
            pltpu.VMEM((STEPS, 8, 128), f32),
            pltpu.SemaphoreType.DMA((3,)),
            pltpu.SemaphoreType.DMA((2, chunks)),
            pltpu.SemaphoreType.DMA((2, chunks)),
            pair,
            pair,
            pair,
            pair,
            pltpu.SemaphoreType.DMA((2, 2 * chunks)),
            pltpu.SemaphoreType.DMA((2, 2 * chunks)),
            pair,
            pair,
            pltpu.SemaphoreType.DMA((STEPS,)),
            pltpu.SemaphoreType.DMA((STEPS,)),
        ],
        compiler_params=pltpu.CompilerParams(
            collective_id=0, has_side_effects=True, vmem_limit_bytes=40 * 1024 * 1024
        ),
    )(*[placed(value, pltpu.HBM) for value in (dosage, zscores, band_reach)])
    ld_tiles, smoothed, quadratic = pl.pallas_call(
        finish,
        out_shape=(
            jax.ShapeDtypeStruct((width, (2 * BAND + 1) * width), bf16),
            jax.ShapeDtypeStruct((width,), f32),
            jax.ShapeDtypeStruct((1, 1), f32),
        ),
        in_specs=[vmem, vmem, vmem],
        out_specs=(hbm, hbm, hbm),
        scratch_shapes=[pltpu.SMEM((1, 1), f32), pltpu.SemaphoreType.DMA((WRITES + 2,))],
        compiler_params=pltpu.CompilerParams(vmem_limit_bytes=1024 * 1024),
    )(*[placed(value, pltpu.VMEM) for value in results])
    return ld_tiles, smoothed, quadratic[0, 0]


def solution(mesh):
    count = mesh.devices.size
    line = Mesh(mesh.devices.reshape(count), ("i",))
    return jax.shard_map(
        functools.partial(body, count),
        mesh=line,
        in_specs=(P(None, "i"), P("i"), P()),
        out_specs=(P("i", None), P("i"), P()),
        check_vma=False,
    )
```

```python
import functools

import jax
import jax.numpy as jnp
from jax import lax
from jax.experimental import pallas as pl
from jax.experimental.pallas import tpu as pltpu
from jax.sharding import Mesh
from jax.sharding import PartitionSpec as P

BAND = 2
MESH = pl.DeviceIdType.MESH
CHUNKS = (256, 256, 128, 128)
ROWS = 256
STEP = 128
WRITES = 6
NT = (((1,), (1,)), ((), ()))

NEAR_STEPS = ((16, 2, "flip"), (64, 4, "flip"), (64, 4, "mirror"), (4, 4, "flip"), (4, 4, "mirror"), (32, 2, "flip"))
STEPS = len(NEAR_STEPS) + 2


def partners_of(me, count):
    partners = []
    for stride, size, kind in NEAR_STEPS:
        digit = lax.rem(lax.div(me, stride), size)
        step = 1 - 2 * lax.rem(digit, 2) if kind == "flip" else size - 1 - 2 * digit
        partners.append(me + step * stride)
    step = 1 - 2 * lax.rem(me, 2)
    partners.append(me + step)
    partners.append(lax.rem(me - step + count, count))
    return partners


def column_stats(source, columns, samples):
    width = columns.size

    def add(step, total):
        rows = pl.ds(pl.multiple_of(step * STEP, STEP), STEP)
        values = source[rows, columns].astype(jnp.float32)
        return total + values.reshape(STEP // 8, 8, width).sum(axis=0)

    zero = jnp.zeros((8, width), jnp.float32)
    total = lax.fori_loop(0, samples // STEP, add, zero)
    mean = jnp.sum(total, axis=0, keepdims=True) / samples

    def add_square(step, total):
        rows = pl.ds(pl.multiple_of(step * STEP, STEP), STEP)
        centered = source[rows, columns].astype(jnp.float32) - mean
        return total + (centered * centered).reshape(STEP // 8, 8, width).sum(axis=0)

    total = lax.fori_loop(0, samples // STEP, add_square, zero)
    variance = jnp.sum(total, axis=0, keepdims=True) / samples
    return mean, lax.rsqrt(variance + 1e-05)


def standardize(source, plain, turned, columns, samples):
    mean, inverse = column_stats(source, columns, samples)

    def write(step, carry):
        rows = pl.ds(pl.multiple_of(step * STEP, STEP), STEP)
        values = (source[rows, columns].astype(jnp.float32) - mean) * inverse
        plain[rows, columns] = values.astype(jnp.bfloat16)
        turned[columns, rows] = values.T.astype(jnp.bfloat16)
        return carry

    lax.fori_loop(0, samples // STEP, write, 0)


def kernel(
    count,
    x_hbm,
    z_hbm,
    reach_hbm,
    out_ref,
    smooth_ref,
    quad_ref,
    own,
    own_scores,
    reach_ref,
    rx,
    plain,
    turned,
    tx,
    left_z,
    right_z,
    own_row,
    own_u,
    near_u,
    tx_smooth,
    rx_smooth,
    partial,
    swapped,
    load_sem,
    send_sem,
    recv_sem,
    z_send,
    z_recv,
    u_send,
    u_recv,
    tile_send,
    tile_recv,
    smooth_send,
    smooth_recv,
    sum_send,
    sum_recv,
):
    me = lax.axis_index("i")
    samples, width = x_hbm.shape
    starts = [sum(CHUNKS[:index]) for index in range(len(CHUNKS))]
    left, right = lax.rem(me + count - 1, count), lax.rem(me + 1, count)
    sides = (left, right)
    partners = partners_of(me, count)

    loads = [
        pltpu.make_async_copy(source, target, load_sem.at[index])
        for index, (source, target) in enumerate(
            ((x_hbm, own), (z_hbm, own_scores), (reach_hbm, reach_ref))
        )
    ]
    for load in loads:
        load.start()
    barrier = pltpu.get_barrier_semaphore()
    peers = sides + tuple(partners[: len(NEAR_STEPS)])
    for device in peers:
        pl.semaphore_signal(barrier, inc=1, device_id=(device,), device_id_type=MESH)
    pl.semaphore_wait(barrier, len(peers))

    def to_side(side, source, target, send, recv):
        return pltpu.make_async_remote_copy(
            src_ref=source,
            dst_ref=target,
            send_sem=send.at[side],
            recv_sem=recv.at[1 - side],
            device_id=(sides[side],),
            device_id_type=MESH,
        )

    def started(copies):
        for copy in copies:
            copy.start()
        return copies

    def chunk_copy(side, chunk):
        columns = pl.ds(starts[chunk], CHUNKS[chunk])
        return pltpu.make_async_remote_copy(
            src_ref=x_hbm.at[:, columns],
            dst_ref=rx.at[1 - side, :, columns],
            send_sem=send_sem.at[side, chunk],
            recv_sem=recv_sem.at[1 - side, chunk],
            device_id=(sides[side],),
            device_id_type=MESH,
        )

    near_z = (left_z, right_z)
    z_copies = started(
        [to_side(side, z_hbm, near_z[1 - side], z_send, z_recv) for side in range(2)]
    )
    chunk_copies = [
        [chunk_copy(side, chunk) for side in range(2)] for chunk in range(len(CHUNKS))
    ]
    started(chunk_copies[0])
    for load in loads:
        load.wait()

    def reach_of(block):
        inside = (block >= 0) & (block < count)
        value = reach_ref[jnp.clip(block, 0, count - 1)]
        return jnp.where(inside, value, -1)

    def factor(first, second, offset):
        allowed = jnp.minimum(reach_of(first), reach_of(second)) >= offset
        return jnp.where(allowed, jnp.float32(1.0), jnp.float32(0.0)) / samples

    near_factor = (factor(me, me - 1, 1), factor(me, me + 1, 1))
    far_factor = factor(me - 1, me + 1, 2)
    own_factor = factor(me, me, 0)

    def as_row(scores):
        return scores[...].astype(jnp.float32).reshape(1, width)

    def as_matrix(scores):
        return jnp.broadcast_to(scores, (8, width)).astype(jnp.bfloat16)

    for start in range(0, width, ROWS):
        standardize(own, plain.at[2], turned.at[2], pl.ds(start, ROWS), samples)
    own_u[...] = jnp.dot(
        as_matrix(as_row(own_scores)), turned[2], preferred_element_type=jnp.float32
    )[0:1, :]

    def into_middle(slot, columns, offset, scale):
        def rows_of(step, carry):
            rows = pl.ds(pl.multiple_of(step * ROWS, ROWS), ROWS)
            product = jnp.dot(
                turned[2, rows, :], plain[slot, :, columns], preferred_element_type=jnp.float32
            )
            place = pl.ds((BAND + offset) * width + columns.start, columns.size)
            out_ref[rows, place] = (product * scale).astype(jnp.bfloat16)
            return carry

        lax.fori_loop(0, width // ROWS, rows_of, 0)

    into_middle(2, pl.ds(0, ROWS), 0, own_factor)
    u_copies = started(
        [to_side(side, own_u, near_u.at[1 - side], u_send, u_recv) for side in range(2)]
    )
    started(chunk_copies[1])
    for start in range(ROWS, width, ROWS):
        into_middle(2, pl.ds(start, ROWS), 0, own_factor)

    def applied(scores, tile):
        return lax.dot_general(
            as_matrix(scores), tile, NT, preferred_element_type=jnp.float32
        )[0:1, :]

    own_row[...] = applied(as_row(own_scores), out_ref[:, pl.ds(BAND * width, width)])

    def sum_copy(step):
        return pltpu.make_async_remote_copy(
            src_ref=partial.at[step],
            dst_ref=swapped.at[step],
            send_sem=sum_send.at[step],
            recv_sem=sum_recv.at[step],
            device_id=(partners[step],),
            device_id_type=MESH,
        )

    sum_copies = [sum_copy(step) for step in range(STEPS)]

    def finish_step(step):
        sum_copies[step].wait_recv()
        partial[step + 1] = partial[step] + swapped[step]

    def tile_copy(side, index, rows, columns):
        place = 2 * BAND * width if side == 0 else 0
        return pltpu.make_async_remote_copy(
            src_ref=tx.at[side, rows, columns],
            dst_ref=out_ref.at[rows, pl.ds(place + columns.start, columns.size)],
            send_sem=tile_send.at[side, index],
            recv_sem=tile_recv.at[1 - side, index],
            device_id=(sides[side],),
            device_id_type=MESH,
        )

    tile_copies = []
    ready = []
    for chunk, (start, size) in enumerate(zip(starts, CHUNKS)):
        columns = pl.ds(start, size)
        for side in range(2):
            chunk_copies[chunk][1 - side].wait_recv()
            if chunk < 2 and side == 1:
                started(chunk_copies[chunk + 2])
            standardize(rx.at[side], plain.at[side], turned.at[side], columns, samples)
        pieces = [(columns, pl.ds(0, start + size))]
        if chunk:
            pieces.append((pl.ds(0, start), columns))
        for rows, across in pieces:
            for side in range(2):
                product = jnp.dot(
                    turned[side, rows, :],
                    plain[1 - side, :, across],
                    preferred_element_type=jnp.float32,
                )
                tx[side, rows, across] = (product * far_factor).astype(jnp.bfloat16)
        ready += [
            tile_copy(side, 2 * chunk + index, rows, across)
            for index, (rows, across) in enumerate(pieces)
            for side in range(2)
        ]
        if chunk < len(CHUNKS) - 1:
            for side in range(2):
                into_middle(side, columns, 2 * side - 1, near_factor[side])
        if chunk == 0:
            for copy in u_copies:
                copy.wait_recv()
            share = near_factor[1] * own_u[...] * near_u[1] + far_factor * near_u[0] * near_u[1]
            total = 2.0 * jnp.sum(share, axis=1, keepdims=True)
            total = total + jnp.sum(as_row(own_scores) * own_row[...], axis=1, keepdims=True)
            partial[0] = jnp.broadcast_to(total, (8, 128))
            started(sum_copies[:1])
        if chunk == len(CHUNKS) - 2:
            finish_step(STEPS - 3)
            started(sum_copies[STEPS - 2 : STEPS - 1])
        if chunk < len(CHUNKS) - 1:
            tile_copies += started(ready)
            ready = []
        if chunk == 0:
            finish_step(0)
            for step in range(1, STEPS - 3):
                started(sum_copies[step : step + 1])
                finish_step(step)
            started(sum_copies[STEPS - 3 : STEPS - 2])

    for copy in z_copies:
        copy.wait_recv()
    near_z = [as_row(scores) for scores in near_z]
    for side in range(2):
        tx_smooth[side] = applied(near_z[1 - side], tx[side])
    smooth_copies = started(
        [
            to_side(side, tx_smooth.at[side], rx_smooth.at[1 - side], smooth_send, smooth_recv)
            for side in range(2)
        ]
    )
    tile_copies += started(ready[:2])
    finish_step(STEPS - 2)
    started(sum_copies[STEPS - 1 :])
    tile_copies += started(ready[2:])
    row = own_row[...]
    for side in range(2):
        into_middle(side, columns, 2 * side - 1, near_factor[side])
        place = pl.ds((BAND + 2 * side - 1) * width, width)
        row = row + applied(near_z[side], out_ref[:, place])
    finish_step(STEPS - 1)
    quad_ref[...] = partial[STEPS] / (count * width)
    for copy in smooth_copies:
        copy.wait_recv()
    row = row + rx_smooth[0] + rx_smooth[1]
    smooth_ref[...] = row.reshape(width)
    for copy in tile_copies:
        copy.wait_recv()
    for pair in chunk_copies:
        for copy in pair:
            copy.wait_send()
    for copy in z_copies + u_copies + tile_copies + smooth_copies + sum_copies:
        copy.wait_send()


def finish(tiles_ref, smooth_ref, quad_ref, tiles_hbm, smooth_hbm, quad_hbm, quad, sems):
    rows = tiles_ref.shape[0] // WRITES
    copies = []
    for index in range(WRITES):
        place = pl.ds(index * rows, rows)
        copies.append(
            pltpu.make_async_copy(tiles_ref.at[place], tiles_hbm.at[place], sems.at[index])
        )
    copies.append(pltpu.make_async_copy(smooth_ref, smooth_hbm, sems.at[WRITES]))
    copies.append(pltpu.make_async_copy(quad, quad_hbm, sems.at[WRITES + 1]))
    for copy in copies[:-1]:
        copy.start()
    quad[0, 0] = quad_ref[0, 0]
    copies[-1].start()
    for copy in copies:
        copy.wait()


def body(count, dosage, zscores, band_reach):
    samples, width = dosage.shape
    chunks = len(CHUNKS)
    bf16, f32 = jnp.bfloat16, jnp.float32
    vmem = pl.BlockSpec(memory_space=pltpu.VMEM)
    hbm = pl.BlockSpec(memory_space=pltpu.HBM)
    placed = pltpu.with_memory_space_constraint
    pair = pltpu.SemaphoreType.DMA((2,))
    results = pl.pallas_call(
        functools.partial(kernel, count),
        out_shape=(
            pltpu.VMEM((width, (2 * BAND + 1) * width), bf16),
            pltpu.VMEM((width,), f32),
            pltpu.VMEM((8, 128), f32),
        ),
        in_specs=[hbm, hbm, hbm],
        out_specs=(vmem, vmem, vmem),
        scratch_shapes=[
            pltpu.VMEM((samples, width), bf16),
            pltpu.VMEM((width,), bf16),
            pltpu.SMEM((count,), jnp.int32),
            pltpu.VMEM((2, samples, width), bf16),
            pltpu.VMEM((3, samples, width), bf16),
            pltpu.VMEM((3, width, samples), bf16),
            pltpu.VMEM((2, width, width), bf16),
            pltpu.VMEM((width,), bf16),
            pltpu.VMEM((width,), bf16),
            pltpu.VMEM((1, width), f32),
            pltpu.VMEM((1, samples), f32),
            pltpu.VMEM((2, 1, samples), f32),
            pltpu.VMEM((2, 1, width), f32),
            pltpu.VMEM((2, 1, width), f32),
            pltpu.VMEM((STEPS + 1, 8, 128), f32),
            pltpu.VMEM((STEPS, 8, 128), f32),
            pltpu.SemaphoreType.DMA((3,)),
            pltpu.SemaphoreType.DMA((2, chunks)),
            pltpu.SemaphoreType.DMA((2, chunks)),
            pair,
            pair,
            pair,
            pair,
            pltpu.SemaphoreType.DMA((2, 2 * chunks)),
            pltpu.SemaphoreType.DMA((2, 2 * chunks)),
            pair,
            pair,
            pltpu.SemaphoreType.DMA((STEPS,)),
            pltpu.SemaphoreType.DMA((STEPS,)),
        ],
        compiler_params=pltpu.CompilerParams(
            collective_id=0, has_side_effects=True, vmem_limit_bytes=40 * 1024 * 1024
        ),
    )(*[placed(value, pltpu.HBM) for value in (dosage, zscores, band_reach)])
    ld_tiles, smoothed, quadratic = pl.pallas_call(
        finish,
        out_shape=(
            jax.ShapeDtypeStruct((width, (2 * BAND + 1) * width), bf16),
            jax.ShapeDtypeStruct((width,), f32),
            jax.ShapeDtypeStruct((1, 1), f32),
        ),
        in_specs=[vmem, vmem, vmem],
        out_specs=(hbm, hbm, hbm),
        scratch_shapes=[pltpu.SMEM((1, 1), f32), pltpu.SemaphoreType.DMA((WRITES + 2,))],
        compiler_params=pltpu.CompilerParams(vmem_limit_bytes=1024 * 1024),
    )(*[placed(value, pltpu.VMEM) for value in results])
    return ld_tiles, smoothed, quadratic[0, 0]


def solution(mesh):
    count = mesh.devices.size
    line = Mesh(mesh.devices.reshape(count), ("i",))
    return jax.shard_map(
        functools.partial(body, count),
        mesh=line,
        in_specs=(P(None, "i"), P("i"), P()),
        out_specs=(P("i", None), P("i"), P()),
        check_vma=False,
    )
```
